32 devices in a mesh: row: 4 (over x, core), col: 8 (over z, y).
Axes of the slice: x: 2, y: 2, z: 4, core: 2. Of those that a mesh axis runs over, the one named last changes fastest.
Arguments:
- velocity_start: float32 [2, 256, 1024], P(None, 'row', 'col'), may hold values from -3 to 3
- stress_start: float32 [3, 256, 1024], P(None, 'row', 'col'), may hold values from -3 to 3
- wind_stress: float32 [2, 256, 1024], P(None, 'row', 'col'), may hold values from -6 to 6
- ocean_current: float32 [2, 256, 1024], P(None, 'row', 'col'), may hold values from -3 to 3
- ice_area: float32 [5, 256, 1024], P(None, 'row', 'col'), may hold values from 0.15 to 0.2
- ice_volume: float32 [5, 256, 1024], P(None, 'row', 'col'), may hold values from 0.05 to 0.6
- inverse_width: float32 [256, 1024], P('row', 'col'), may hold values from 0.7 to 1.4
- inverse_height: float32 [256, 1024], P('row', 'col'), may hold values from 0.7 to 1.4
- land_block: int32 [64, 32], P('row', 'col'), may hold values 0 or 1
- ice_block: int32 [64, 32], P('row', 'col'), may hold values 0 or 1
- writer: int32 [8], replicated, may hold values from 0 to 3
Outputs:
- velocity: float32 [2, 256, 1024], P(None, 'row', 'col')
- stress: float32 [3, 256, 1024], P(None, 'row', 'col')
- restart: float32 [4, 10, 256, 1024], P('row', None, None, 'col')
The draws below stay inside these ranges and needn't reach their ends.
All inputs are finite; a program needn't handle non-finite values. No bound on the sum of `land_block` or of `ice_block` on one device may be relied on, other than what follows from the above.
Results may differ from the reference program's by a relative error of at most 0.00002.
Values sent between devices are 32-bit elements; how exact they have to be, the bound alone decides.
A program may use at most 64 MiB of HBM per device.

```python
import math
import jax
import jax.numpy as jnp
from jax import lax

CX = 128
NCAT = 5
SUB = 12
NY = 256
NX = 1024
NBY = 64
NBX = 32
GROUPS = 8
SLOTS = 4


def place_ends(array, key, least, high):
    spot = [jax.random.randint(jax.random.fold_in(key, axis), (), 0, length) for axis, length in enumerate(array.shape)]
    longest = array.shape.index(max(array.shape))
    neighbour = spot[:longest] + [(spot[longest] + 1) % array.shape[longest]] + spot[longest + 1:]
    return array.at[tuple(spot)].set(least).at[tuple(neighbour)].set(high)


def block_scale(rng, extent, pieces, least, largest):
    gain, own = 1.0, jax.random.fold_in(rng, 6)
    for axis_at, shards_of in pieces:
        draws = jnp.exp(jax.random.uniform(jax.random.fold_in(own, axis_at), (shards_of,), jnp.float32, least / len(pieces), largest / len(pieces)))
        gain = gain * jnp.repeat(draws, extent[axis_at] // shards_of).reshape([-1 if axis == axis_at else 1 for axis in range(len(extent))])
    return gain


def centred(stream_key, shape, scale, reach, cuts=(), held_as=jnp.bfloat16):
    array = jax.random.normal(stream_key, shape, jnp.float32) * scale
    if len(cuts) > 0:
        array = block_scale(stream_key, shape, cuts, -0.22, 0.18) * array
    return jnp.clip(array, min=-reach, max=reach).astype(held_as)


def setup_inputs(seed: int = 0) -> dict:
    splits = jax.random.split(jax.random.key(seed), 12)
    velocity_start = centred(splits[0], (2, NY, NX), 0.5, 3.0, ((1, 4), (2, 8)), jnp.float32)
    stress_start = centred(splits[1], (3, NY, NX), 0.5, 3.0, ((1, 4), (2, 8)), jnp.float32)
    wind_stress = centred(splits[2], (2, NY, NX), 1.0, 6.0, ((1, 4), (2, 8)), jnp.float32)
    ocean_current = centred(splits[3], (2, NY, NX), 0.5, 3.0, ((1, 4), (2, 8)), jnp.float32)
    ice_area = jnp.clip(0.15 + 0.049999997 * jax.random.uniform(splits[4], (NCAT, NY, NX), jnp.float32) ** block_scale(splits[4], (NCAT, NY, NX), ((1, 4), (2, 8)), -0.2, 0.2), 0.15, 0.2)
    ice_volume = jnp.clip(0.05 + 0.55 * jax.random.uniform(splits[5], (NCAT, NY, NX), jnp.float32) ** block_scale(splits[5], (NCAT, NY, NX), ((1, 4), (2, 8)), -0.2, 0.2), 0.05, 0.6)
    inverse_width = jnp.clip(jnp.exp(math.log(1.4) - 0.6931472 * jax.random.uniform(splits[6], (NY, NX), jnp.float32) ** block_scale(splits[6], (NY, NX), ((0, 4), (1, 8)), -0.2, 0.2)), 0.7, 1.4)
    inverse_height = jnp.clip(jnp.exp(math.log(1.4) - 0.6931472 * jax.random.uniform(splits[7], (NY, NX), jnp.float32) ** block_scale(splits[7], (NY, NX), ((0, 4), (1, 8)), -0.2, 0.2)), 0.7, 1.4)
    land_block = place_ends((jax.random.randint(splits[8], (NBY, NBX), 0, 4) < 3).astype(jnp.int32), jax.random.fold_in(splits[8], 1), 0, 1)
    ice_block = place_ends((jax.random.randint(splits[9], (NBY, NBX), 0, 3) < 2).astype(jnp.int32), jax.random.fold_in(splits[9], 1), 0, 1)
    writer = place_ends(jax.random.randint(splits[10], (GROUPS,), 0, SLOTS), jax.random.fold_in(splits[10], 1), 0, SLOTS - 1).astype(jnp.int32)
    return {"velocity_start": velocity_start, "stress_start": stress_start, "wind_stress": wind_stress, "ocean_current": ocean_current, "ice_area": ice_area, "ice_volume": ice_volume, "inverse_width": inverse_width, "inverse_height": inverse_height, "land_block": land_block, "ice_block": ice_block, "writer": writer}


strength_scale = 4.0
hibler_decay = 20.0
mass_rate = 16.0
water_drag = 1.0
coriolis = 0.5
relax_rate = 0.5
ellipse_square = 4.0
delta_margin = 0.5

def expand_blocks(blocks, height, breadth):
    counted = blocks.astype(jnp.float32)
    block_rows, block_cols = counted.shape
    spread = jnp.broadcast_to(counted[:, None, :, None], (block_rows, height // block_rows, block_cols, breadth // block_cols))
    return spread.reshape(height, breadth)

def stress_update(stresses, strength, across_scale, along_scale, north_east, north_west, south_east, south_west):
    grad_ux = 0.5 * across_scale * (north_east[0] + south_east[0] - (north_west[0] + south_west[0]))
    grad_vy = 0.5 * along_scale * (north_east[1] + north_west[1] - (south_east[1] + south_west[1]))
    grad_uy = 0.5 * along_scale * (north_east[0] + north_west[0] - (south_east[0] + south_west[0]))
    grad_vx = 0.5 * across_scale * (north_east[1] + south_east[1] - (north_west[1] + south_west[1]))
    divergence = grad_ux + grad_vy
    tension = grad_ux - grad_vy
    shearing = grad_uy + grad_vx
    deform = jnp.sqrt(divergence * divergence + (tension * tension + shearing * shearing) / ellipse_square)
    viscous = strength / (deform + delta_margin)
    normal_sum = (stresses[0] + relax_rate * viscous * (divergence - deform)) / (1.0 + relax_rate)
    normal_diff = (stresses[1] + relax_rate * viscous * tension / ellipse_square) / (1.0 + relax_rate)
    shear_new = (stresses[2] + relax_rate * viscous * shearing / (2.0 * ellipse_square)) / (1.0 + relax_rate)
    return jnp.stack([normal_sum, normal_diff, shear_new])

def normal_xx(stresses):
    return 0.5 * (stresses[0] + stresses[1])

def normal_yy(stresses):
    return 0.5 * (stresses[0] - stresses[1])

def stress_force(across_scale, along_scale, south_west, south_east, north_west, north_east):
    force_x = 0.5 * across_scale * (normal_xx(south_east) + normal_xx(north_east) - (normal_xx(south_west) + normal_xx(north_west))) + 0.5 * along_scale * (north_west[2] + north_east[2] - (south_west[2] + south_east[2]))
    force_y = 0.5 * across_scale * (south_east[2] + north_east[2] - (south_west[2] + north_west[2])) + 0.5 * along_scale * (normal_yy(north_west) + normal_yy(north_east) - (normal_yy(south_west) + normal_yy(south_east)))
    return (force_x, force_y)

def momentum(velocity, force_x, force_y, inertia, turning, wind_stress, ocean_current, land_cells, ice_cells):
    damped = inertia + water_drag
    right_x = inertia * velocity[0] + force_x + wind_stress[0] + water_drag * ocean_current[0]
    right_y = inertia * velocity[1] + force_y + wind_stress[1] + water_drag * ocean_current[1]
    denominator = damped * damped + turning * turning
    next_u = (damped * right_x + turning * right_y) / denominator
    next_v = (damped * right_y - turning * right_x) / denominator
    moving = jnp.stack([next_u, next_v])
    return land_cells * (ice_cells * moving + (1.0 - ice_cells) * ocean_current)

def shift_south(stacked):
    return jnp.concatenate([jnp.zeros_like(stacked[:, :1]), stacked[:, :-1]], axis=1)

def fold_north(stacked):
    return jnp.concatenate([stacked[:, 1:], stacked[:, -1:, ::-1]], axis=1)

def reference(velocity_start, stress_start, wind_stress, ocean_current, ice_area, ice_volume, inverse_width, inverse_height, land_block, ice_block, writer):
    height, breadth = inverse_width.shape
    land_cells = expand_blocks(land_block, height, breadth)
    ice_cells = expand_blocks(ice_block, height, breadth)
    area_total = lax.optimization_barrier(jnp.sum(ice_area, axis=0))
    volume_total = lax.optimization_barrier(jnp.sum(ice_volume, axis=0))
    strength = strength_scale * volume_total * jnp.exp(-hibler_decay * (1.0 - area_total)) * land_cells
    inertia = mass_rate * (1.0 + volume_total)
    turning = coriolis * (1.0 + volume_total)
    velocity = velocity_start
    stresses = stress_start
    for subcycle in range(SUB):
        west_side = jnp.roll(velocity, 1, axis=2)
        south_side = shift_south(velocity)
        south_west = shift_south(west_side)
        stresses = stress_update(stresses, strength, inverse_width, inverse_height, velocity, west_side, south_side, south_west)
        east_side = jnp.roll(stresses, -1, axis=2)
        north_side = fold_north(stresses)
        north_east = jnp.roll(north_side, -1, axis=2)
        force_x, force_y = stress_force(inverse_width, inverse_height, stresses, east_side, north_side, north_east)
        velocity = momentum(velocity, force_x, force_y, inertia, turning, wind_stress, ocean_current, land_cells, ice_cells)
    snapshot = jnp.concatenate([ice_area, ice_volume], axis=0)
    strip_owner = writer[jnp.arange(NX, dtype=jnp.int32) // CX]
    slot_index = jnp.arange(SLOTS, dtype=jnp.int32)
    chosen = slot_index[:, None, None, None] == strip_owner[None, None, None, :]
    restart = jnp.where(chosen, snapshot[None], jnp.zeros((), snapshot.dtype))
    return (velocity, stresses, restart)
```

```python
import functools

import jax
import jax.numpy as jnp
from jax import lax
from jax.experimental import pallas as pl
from jax.experimental.pallas import tpu as pltpu
from jax.sharding import PartitionSpec as P

SUB = 12
PAD = 8
FIELDS = 11
STORED = 14
U, V, S, D, T, GU, GV, INERTIA, STRENGTH, HW, HH, BETA, FW, FH = range(STORED)
ALPHA = INERTIA
TINY = 1.1754944e-38

strength_scale = 4.0
hibler_decay = 20.0
mass_rate = 16.0
water_drag = 1.0
coriolis = 0.5


def halo_rows():
    return -(-SUB // 8) * 8


def slots_of(breadth):
    return breadth // SUB


def region(breadth):
    return -(-(halo_rows() // 8) * FIELDS // slots_of(breadth))


def packing(groups, breadth):
    per, tiles, deep = slots_of(breadth), region(breadth), halo_rows() // 8
    where = {}
    for k in range(deep):
        for f in range(FIELDS):
            n = k * FIELDS + f
            where[k, f] = divmod(n, per)
            where[groups - 1 - k, f] = (tiles + n // per, n % per)
    spare = [divmod(n, per) for n in range(deep * FIELDS, tiles * per)]
    free = spare + [(tiles + t, n) for t, n in spare]
    n = 0
    for k in range(deep, groups - deep):
        for f in range(FIELDS):
            m = n - len(free)
            where[k, f] = free[n] if m < 0 else (2 * tiles + m // per, m % per)
            n += 1
    return where, 1 + max(t for t, _ in where.values())


def expand_into(mask_ref, blocks_ref):
    block_cols, block_rows = blocks_ref.shape
    height, breadth = mask_ref.shape
    tall, wide = height // block_rows, breadth // block_cols
    counted = blocks_ref[...].astype(jnp.float32)
    start = wide * lax.broadcasted_iota(jnp.int32, (block_cols, breadth), 0)
    lane = lax.broadcasted_iota(jnp.int32, (block_cols, breadth), 1)
    inside = (lane >= start) & (lane < start + wide)
    for b in range(block_rows):
        spread = jnp.where(inside, counted[:, b : b + 1], 0.0)
        line = jnp.sum(spread, axis=0, keepdims=True)
        mask_ref[b * tall : (b + 1) * tall, :] = jnp.broadcast_to(line, (tall, breadth))


def kernel(
    nr,
    nc,
    vel_in,
    str_in,
    wind_in,
    cur_in,
    area_in,
    vol_in,
    iw_in,
    ih_in,
    land_in,
    ice_in,
    writer_in,
    vel_out,
    str_out,
    strips,
    writer_out,
    vel_ref,
    str_ref,
    wind_ref,
    cur_ref,
    iw_ref,
    ih_ref,
    land_ref,
    ice_ref,
    vals,
    main,
    side,
    pack_e,
    pack_w,
    land_n,
    land_s,
    mid_e,
    mid_w,
    low_e,
    low_w,
    high_e,
    high_w,
    ocean_ref,
    icy_ref,
    send_sem,
    recv_sem,
    x_send,
    x_recv,
    f_send,
    f_recv,
    in_sem,
    strip_sem,
    ring_sem,
):
    hr = halo_rows()
    height, breadth = iw_ref.shape
    cats = area_in.shape[0]
    rows = height + 2 * hr
    deep = hr // 8
    groups = height // 8
    total = rows // 8
    half = breadth // 2
    skip = total // 2 - deep
    tall = total - skip
    base = breadth - half + SUB
    cut = (base + breadth - SUB) // 2
    where, _ = packing(groups, breadth)
    tiles = region(breadth)
    r = lax.axis_index("row")
    c = lax.axis_index("col")
    east = lax.rem(c + 1, nc)
    west = lax.rem(c + nc - 1, nc)
    mirror = nc - 1 - c
    m_e = lax.rem(mirror + nc - 1, nc)
    m_w = lax.rem(mirror + 1, nc)
    partner = r + 1 - 2 * lax.rem(r, 2)
    is_top = r == nr - 1
    not_top = r < nr - 1
    above_bottom = r > 0
    self_e = jnp.logical_and(is_top, m_e == c)
    self_w = jnp.logical_and(is_top, m_w == c)
    other_e = jnp.logical_and(is_top, m_e != c)
    other_w = jnp.logical_and(is_top, m_w != c)
    others = [lax.rem(r + 2 * k, nr) for k in range(1, nr // 2)]

    own = pl.ds(pl.multiple_of(r * height, height), height)
    area_own = strips.at[0:cats, own, :]
    vol_own = strips.at[cats : 2 * cats, own, :]
    inputs = (
        (area_in, area_own),
        (vol_in, vol_own),
        (land_in, land_ref),
        (ice_in, ice_ref),
        (vel_in, vel_ref),
        (str_in, str_ref),
        (wind_in, wind_ref),
        (cur_in, cur_ref),
        (iw_in, iw_ref),
        (ih_in, ih_ref),
        (writer_in, writer_out),
    )
    arriving = [
        pltpu.make_async_copy(src, dst, in_sem.at[n]) for n, (src, dst) in enumerate(inputs)
    ]
    for copy in arriving:
        copy.start()

    barrier = pltpu.get_barrier_semaphore()

    def signal(semaphore, row, col):
        pl.semaphore_signal(
            semaphore,
            inc=1,
            device_id={"row": row, "col": col},
            device_id_type=pl.DeviceIdType.MESH,
        )

    odd = lax.rem(r, 2) == 1
    even = lax.rem(r, 2) == 0
    floor = r - lax.rem(r, 2)
    up_chip = jnp.logical_and(odd, not_top)
    down_chip = jnp.logical_and(even, above_bottom)
    along_x = jnp.logical_or(up_chip, down_chip)
    for n in range(nr // 2):
        chief = 2 * n + 1

        @pl.when(r != chief)
        def _():
            signal(barrier, chief, c)

    for beside in (east, west):
        signal(barrier, floor, beside)

        @pl.when(up_chip)
        def _():
            signal(barrier, r + 1, beside)

        @pl.when(down_chip)
        def _():
            signal(barrier, r - 2, beside)

    @pl.when(is_top)
    def _():
        signal(barrier, floor, mirror)

    @pl.when(other_e)
    def _():
        signal(barrier, floor, m_e)

    @pl.when(other_w)
    def _():
        signal(barrier, floor, m_w)

    def remote(src, dst, send, recv, row, col):
        return pltpu.make_async_remote_copy(
            src_ref=src,
            dst_ref=dst,
            send_sem=send,
            recv_sem=recv,
            device_id={"row": row, "col": col},
            device_id_type=pl.DeviceIdType.MESH,
        )

    snapshot = (area_own, vol_own)
    crossing = []
    for k, other in enumerate(others):
        for part, ref in enumerate(snapshot):
            n = 2 * k + part
            crossing.append(remote(ref, ref, x_send.at[n], x_recv.at[n], other, c))
    forwards = [
        remote(ref, ref, f_send.at[part], f_recv.at[part], partner, c)
        for part, ref in enumerate(snapshot)
    ]

    lane = lax.broadcasted_iota(jnp.int32, (8, breadth), 1)
    sub = lax.broadcasted_iota(jnp.int32, (8, breadth), 0)
    zero = jnp.zeros((8, breadth), jnp.float32)
    left_half = lane < half
    for f in range(5):
        for ref, end in ((main, PAD + rows), (side, PAD + 8 * tall)):
            ref[f, 0:PAD, :] = zero
            ref[f, end : end + PAD, :] = zero

    def roll(value, shift):
        shift = shift % breadth
        return pltpu.roll(value, shift, 1) if shift else value

    for copy in arriving:
        copy.wait()
    expand_into(ocean_ref, land_ref)
    expand_into(icy_ref, ice_ref)
    packed_e, packed_w = {}, {}
    order = list(range(deep)) + list(range(groups - 1, groups - 1 - deep, -1))
    order += list(range(deep, groups - deep))
    for k in order:
        here = slice(8 * k, 8 * k + 8)
        lines = pl.ds(pl.multiple_of(r * height + 8 * k, 8), 8)
        area = strips[0, lines, :]
        volume = strips[cats, lines, :]
        for n in range(1, cats):
            area = area + strips[n, lines, :]
            volume = volume + strips[cats + n, lines, :]
        ocean = ocean_ref[here, :]
        icy = icy_ref[here, :]
        strength = strength_scale * volume * jnp.exp(-hibler_decay * (1.0 - area)) * ocean
        inertia = mass_rate * (1.0 + volume)
        turning = coriolis * (1.0 + volume)
        damped = inertia + water_drag
        moving = ocean * icy
        live = moving / (damped * damped + turning * turning)
        ca = damped * live
        cb = turning * live
        rest = ocean * (1.0 - icy)
        cu = cur_ref[0, here, :]
        cv = cur_ref[1, here, :]
        gu = wind_ref[0, here, :] + water_drag * cu
        gv = wind_ref[1, here, :] + water_drag * cv
        s1, s2 = str_ref[0, here, :], str_ref[1, here, :]
        values = [
            vel_ref[0, here, :],
            vel_ref[1, here, :],
            s1 + s2,
            s1 - s2,
            2.0 * str_ref[2, here, :],
            ca * gu + cb * gv + rest * cu,
            ca * gv - cb * gu + rest * cv,
            moving * inertia,
            strength * (1.0 / 3.0),
            0.5 * iw_ref[here, :],
            0.5 * ih_ref[here, :],
        ]
        for f, value in enumerate(values):
            vals[f, here, :] = value
            t, n = where[k, f]
            at = n * SUB
            to_w, to_e = roll(value, at), roll(value, at + SUB)
            if t in packed_w:
                to_w = jnp.where(lane >= at, to_w, packed_w[t])
                to_e = jnp.where(lane >= at, to_e, packed_e[t])
            packed_w[t], packed_e[t] = to_w, to_e
    for t in packed_w:
        pack_w[t] = packed_w[t]
        pack_e[t] = packed_e[t]

    @pl.when(odd)
    def _():
        pl.semaphore_wait(barrier, nr - 1)
        signal(strip_sem, partner, c)

    @pl.when(even)
    def _():
        pl.semaphore_wait(strip_sem, 1)

    def halo(slot, src, dst, row, col):
        return remote(src, dst, send_sem.at[slot], recv_sem.at[slot], row, col)

    bottom = slice(0, tiles)
    upper = slice(tiles, 2 * tiles)
    vals_top = vals.at[:, height - hr : height, :]
    vals_bottom = vals.at[:, 0:hr, :]
    to_west = halo(0, pack_w, mid_e, r, west)
    to_east = halo(1, pack_e, mid_w, r, east)
    up = [
        halo(2, vals_top, land_s, r + 1, c),
        halo(4, pack_w.at[upper], low_e, r + 1, west),
        halo(5, pack_e.at[upper], low_w, r + 1, east),
    ]
    down = [
        halo(3, vals_bottom, land_n, r - 1, c),
        halo(6, pack_w.at[bottom], high_e, r - 1, west),
        halo(7, pack_e.at[bottom], high_w, r - 1, east),
    ]
    over = remote(vals_top, land_n, send_sem.at[8], recv_sem.at[3], r, mirror)
    over_w = remote(pack_w.at[upper], high_e, send_sem.at[9], recv_sem.at[6], r, m_w)
    over_e = remote(pack_e.at[upper], high_w, send_sem.at[10], recv_sem.at[7], r, m_e)

    @pl.when(not_top)
    def _():
        up[0].start()

    @pl.when(above_bottom)
    def _():
        down[0].start()

    @pl.when(jnp.logical_not(along_x))
    def _():
        for copy in crossing:
            copy.start()

    for copy in forwards:
        copy.start()

    @pl.when(even)
    def _():
        top_chip = (r == nr - 2).astype(jnp.int32)
        peers = 4 + 2 * above_bottom.astype(jnp.int32) + 2 - 2 * top_chip + top_chip
        peers = peers + top_chip * (m_e != c).astype(jnp.int32)
        peers = peers + top_chip * (m_w != c).astype(jnp.int32)
        pl.semaphore_wait(barrier, peers)
        signal(ring_sem, partner, c)

    @pl.when(odd)
    def _():
        pl.semaphore_wait(ring_sem, 1)

    @pl.when(self_w)
    def _():
        high_e[...] = pack_w[upper]

    @pl.when(self_e)
    def _():
        high_w[...] = pack_e[upper]

    def send_beside(mid, across, other, folded):
        mid.start()

        @pl.when(not_top)
        def _():
            up[across].start()

        @pl.when(above_bottom)
        def _():
            down[across].start()

        @pl.when(other)
        def _():
            folded.start()

    odd_col = lax.rem(c, 2) == 1

    @pl.when(odd_col)
    def _():
        send_beside(to_east, 2, other_e, over_e)

    send_beside(to_west, 1, other_w, over_w)

    @pl.when(jnp.logical_not(odd_col))
    def _():
        send_beside(to_east, 2, other_e, over_e)

    @pl.when(is_top)
    def _():
        over.start()

    @pl.when(along_x)
    def _():
        for copy in crossing:
            copy.start()

    def tile(g):
        return slice(PAD + 8 * g, PAD + 8 * g + 8)

    def homes(g):
        return [(b, n) for b, n in ((g, 0), (g - skip, 1)) if 0 <= b < tall]

    def fill(g, f, value):
        main[f, tile(g), :] = roll(value, SUB)
        for b, right in homes(g):
            mask = lane >= half if right else left_half
            pltpu.store(side.at[f, tile(b), :], roll(value, right * half - base), mask=mask)

    for k in range(groups):
        for f in range(FIELDS):
            fill(deep + k, f, vals[f, 8 * k : 8 * k + 8, :])

    @pl.when(r == 0)
    def _():
        land_s[...] = jnp.zeros(land_s.shape, jnp.float32)
        low_e[...] = jnp.zeros(low_e.shape, jnp.float32)
        low_w[...] = jnp.zeros(low_w.shape, jnp.float32)

    swap = is_top.astype(jnp.int32)

    @pl.when(above_bottom)
    def _():
        up[0].wait_recv()

    @pl.when(not_top)
    def _():
        down[0].wait_recv()

    @pl.when(is_top)
    def _():
        over.wait_recv()

    for g in range(deep):
        line = g + swap * (deep - 1 - 2 * g)
        from_n = pl.ds(pl.multiple_of(8 * line, 8), 8)
        for f in range(FIELDS):
            fill(g, f, land_s[f, 8 * g : 8 * g + 8, :])
            fill(deep + groups + g, f, land_n[f, from_n, :])

    def edges(low, mid, high):
        for g in range(total):
            if g < deep:
                k, source, first = groups - deep + g, low, tiles
            elif g < deep + groups:
                k, source, first = g - deep, mid, 0
            else:
                k, source, first = g - deep - groups, high, 0
            for f in range(FIELDS):
                t, n = where[k, f]
                yield g, f, source[t - first], n * SUB

    to_west.wait_recv()

    @pl.when(above_bottom)
    def _():
        up[1].wait_recv()

    @pl.when(not_top)
    def _():
        down[1].wait_recv()

    @pl.when(other_w)
    def _():
        over_w.wait_recv()

    for g, f, value, at in edges(low_e, mid_e, high_e):
        for b, right in homes(g):
            to = right * half + half - SUB
            mask = (lane >= to) & (lane < to + SUB)
            pltpu.store(side.at[f, tile(b), :], roll(value, to - at), mask=mask)

    to_east.wait_recv()

    @pl.when(above_bottom)
    def _():
        up[2].wait_recv()

    @pl.when(not_top)
    def _():
        down[2].wait_recv()

    @pl.when(other_e)
    def _():
        over_e.wait_recv()

    for g, f, value, at in edges(low_w, mid_w, high_w):
        pltpu.store(main.at[f, tile(g), :], roll(value, -at), mask=lane < SUB)

    turn = coriolis / mass_rate
    for ref, count in ((main, total), (side, tall)):
        for g in range(count):
            here = slice(PAD + 8 * g, PAD + 8 * g + 8)
            inertia = ref[INERTIA, here, :]
            damped = inertia + water_drag
            turning = turn * inertia
            scaled = inertia / (damped * damped + turning * turning)
            inverse = 0.5 / jnp.maximum(inertia, 1.0)
            ref[ALPHA, here, :] = damped * scaled
            ref[BETA, here, :] = turning * scaled
            ref[FW, here, :] = inverse * ref[HW, here, :]
            ref[FH, here, :] = inverse * ref[HH, here, :]

    near = deep + groups
    near_first = PAD + 8 * near
    own_top = near_first - 1
    shift = 8 * skip
    fold_south = (sub == 0) & is_top
    fold_north = (sub == 7) & is_top
    fold_south_side = fold_south & (lane >= half)
    fold_north_side = fold_north & (lane >= half)
    last_line = sub == 7

    def spread(ref, f, at):
        return jnp.broadcast_to(ref[f, at : at + 1, :], (8, breadth))

    def stress_tile(ref, g, folded, far):
        here = slice(PAD + 8 * g, PAD + 8 * g + 8)
        south = slice(PAD + 8 * g - 1, PAD + 8 * g + 7)
        u, v = ref[U, here, :], ref[V, here, :]
        su, sv = ref[U, south, :], ref[V, south, :]
        if folded is not None:
            su = jnp.where(folded, spread(ref, U, far), su)
            sv = jnp.where(folded, spread(ref, V, far), sv)
        us, ud, vs, vd = u + su, u - su, v + sv, v - sv
        du, dv = us - pltpu.roll(us, 1, 1), vs - pltpu.roll(vs, 1, 1)
        eu, ev = ud + pltpu.roll(ud, 1, 1), vd + pltpu.roll(vd, 1, 1)
        hw, hh = ref[HW, here, :], ref[HH, here, :]
        gux, gvy = hw * du, hh * ev
        div, ten, shear = gux + gvy, gux - gvy, hw * dv + hh * eu
        ten4, shear4 = 0.25 * ten, 0.25 * shear
        square = div * div + (ten4 * ten + shear4 * shear)
        deform = square * lax.rsqrt(jnp.maximum(square, TINY))
        w = ref[STRENGTH, here, :] / (deform + 0.5)
        c = div - deform
        ref[S, here, :] = ref[S, here, :] * (2.0 / 3.0) + w * (c + ten4)
        ref[D, here, :] = ref[D, here, :] * (2.0 / 3.0) + w * (c - ten4)
        ref[T, here, :] = ref[T, here, :] * (2.0 / 3.0) + w * shear4

    def velocity_tile(ref, g, folded=None, ghost=None, last=None):
        here = slice(PAD + 8 * g, PAD + 8 * g + 8)
        north = slice(PAD + 8 * g + 1, PAD + 8 * g + 9)
        s, d, t = ref[S, here, :], ref[D, here, :], ref[T, here, :]
        ns, nd, nt = ref[S, north, :], ref[D, north, :], ref[T, north, :]
        if last is not None:
            ns, nd, nt = (
                jnp.where(last_line, spread(ref, f, last), n)
                for f, n in ((S, ns), (D, nd), (T, nt))
            )
        if folded is not None:
            ns, nd, nt = (jnp.where(folded, 0.0, n) for n in (ns, nd, nt))
        ps, dt, pt, dd = s + ns, nt - t, t + nt, nd - d
        back = breadth - 1
        es, et = pltpu.roll(ps, back, 1) - ps, dt + pltpu.roll(dt, back, 1)
        ft, fd = pltpu.roll(pt, back, 1) - pt, dd + pltpu.roll(dd, back, 1)
        if folded is not None:
            es, et, ft, fd = (
                value + jnp.where(folded, line, 0.0)
                for value, line in zip((es, et, ft, fd), ghost)
            )
        fw, fh = ref[FW, here, :], ref[FH, here, :]
        x = ref[U, here, :] + (fw * es + fh * et)
        y = ref[V, here, :] + (fw * ft + fh * fd)
        alpha, beta = ref[ALPHA, here, :], ref[BETA, here, :]
        ref[U, here, :] = alpha * x + beta * y + ref[GU, here, :]
        ref[V, here, :] = alpha * y - beta * x + ref[GV, here, :]

    def mirrored(reach, line):
        index = reach - lane
        return jnp.take_along_axis(line, jnp.where(index < 0, index + breadth, index), axis=1)

    from_side = lane <= breadth - 1 + SUB - cut
    from_side_e = lane < breadth - 1 + SUB - cut

    def fold():
        def stack(ref, back):
            lines = [
                ref[f, at - back : at - back + 1, :]
                for at in (own_top, own_top + 8)
                for f in (S, D, T)
            ]
            return jnp.concatenate(lines + lines[:2], axis=0)

        a, b = stack(main, 0), stack(side, shift)
        last = breadth - 1
        turned, turned_e = mirrored(last, a), mirrored(last - 1, a)
        moved, moved_e = mirrored(last + 2 * SUB, a), mirrored(last - 1 + 2 * SUB, a)
        sides, sides_e = mirrored(last, b), mirrored(last - 1, b)
        moved = jnp.where(from_side, sides, moved)
        moved_e = jnp.where(from_side_e, sides_e, moved_e)
        found = []
        for here, far in ((moved, moved_e), (turned, turned_e)):
            less, more = far - here, far + here
            for first in (3, 0):
                picked = ((less, 0), (more, 2), (less, 2), (more, 1))
                found.append(
                    [
                        jnp.broadcast_to(x[first + f : first + f + 1, :], (8, breadth))
                        for x, f in picked
                    ]
                )
        return found

    def cycle(first, stresses, velocities):
        def body(_, carry):
            for g in range(first, total):
                if g < stresses:
                    on = g == near
                    far = near_first + 15
                    stress_tile(main, g, fold_south if on else None, far)
                    if g < tall - first:
                        on = g == near - skip
                        stress_tile(side, g, fold_south_side if on else None, far - shift)
            ghosts = fold()
            for g in range(first, velocities):
                if g in (near - 1, near):
                    velocity_tile(main, g, fold_north, ghosts[g - near + 1])
                else:
                    velocity_tile(main, g, last=near_first if g == total - 1 else None)
                b = g + skip
                if g < tall - first:
                    if b in (near - 1, near):
                        velocity_tile(side, g, fold_north_side, ghosts[2 + b - near + 1])
                    else:
                        last = near_first - shift if g == tall - 1 else None
                        velocity_tile(side, g, last=last)
            return carry

        return body

    def relay(k, part):
        source = lax.rem(r + nr - 2 * (k + 1), nr)
        lines = pl.ds(pl.multiple_of(source * height, height), height)
        block = strips.at[part * cats : (part + 1) * cats, lines, :]
        slot = 2 + 2 * k + part
        return remote(block, block, f_send.at[slot], f_recv.at[slot], partner, c)

    relays = [relay(k, part) for k in range(len(others)) for part in range(2)]

    def pass_on(parts, early):
        for k in range(len(others)):
            source = lax.rem(r + nr - 2 * (k + 1), nr)
            outer = jnp.logical_or(source == 0, source == nr - 1)

            @pl.when(outer if early else jnp.logical_not(outer))
            def _():
                for part in parts:
                    crossing[2 * k + part].wait_recv()
                    relays[2 * k + part].start()

    wide = SUB - 8
    lax.fori_loop(0, wide, cycle(0, total, total), 0)
    pass_on((0, 1), True)
    lax.fori_loop(0, 4, cycle(1, total - 1, total - 1), 0)
    pass_on((0,), False)
    lax.fori_loop(0, SUB - wide - 5, cycle(1, total - 1, total - 1), 0)
    pass_on((1,), False)
    cycle(1, total - 1, near)(0, 0)

    keep = lane < cut
    for k in range(groups):
        b, right = homes(deep + k)[-1 if 2 * k >= groups else 0]
        out = []
        for f in (U, V, S, D, T):
            a = roll(main[f, tile(deep + k), :], -SUB)
            z = roll(side[f, tile(b), :], base - right * half)
            out.append(jnp.where(keep, a, z))
        at = slice(8 * k, 8 * k + 8)
        vel_out[0, at, :] = out[0]
        vel_out[1, at, :] = out[1]
        str_out[0, at, :] = 0.5 * (out[2] + out[3])
        str_out[1, at, :] = 0.5 * (out[2] - out[3])
        str_out[2, at, :] = 0.5 * out[4]

    to_west.wait_send()
    to_east.wait_send()

    @pl.when(not_top)
    def _():
        for copy in up:
            copy.wait_send()

    @pl.when(above_bottom)
    def _():
        for copy in down:
            copy.wait_send()

    @pl.when(is_top)
    def _():
        over.wait_send()

    @pl.when(other_w)
    def _():
        over_w.wait_send()

    @pl.when(other_e)
    def _():
        over_e.wait_send()

    for copy in crossing:
        copy.wait_send()
    for copy in forwards + relays:
        copy.wait()


def place(strips, vel, stress, writer, restart_out, vel_out, str_out, blank, sem):
    r = lax.axis_index("row")
    c = lax.axis_index("col")
    small = [
        pltpu.make_async_copy(vel, vel_out, sem.at[0]),
        pltpu.make_async_copy(stress, str_out, sem.at[1]),
    ]
    for copy in small:
        copy.start()
    index = lax.broadcasted_iota(jnp.int32, writer.shape, 1)
    chosen = jnp.sum(jnp.where(index == c, writer[...], 0))
    fields = strips.shape[0]

    @pl.when(chosen == r)
    def _():
        copies = [
            pltpu.make_async_copy(strips.at[n], restart_out.at[0, n], sem.at[2 + n])
            for n in range(fields)
        ]
        for copy in copies:
            copy.start()
        for copy in copies:
            copy.wait()

    @pl.when(chosen != r)
    def _():
        blank[...] = jnp.zeros(blank.shape, blank.dtype)
        copies = [
            pltpu.make_async_copy(blank, restart_out.at[0, n], sem.at[2 + n])
            for n in range(fields)
        ]
        for copy in copies:
            copy.start()
        for copy in copies:
            copy.wait()

    for copy in small:
        copy.wait()


def shards(nr, nc, *operands):
    (vel, stress, wind, current, area, volume, iw, ih, land, ice, writer) = operands
    hr = halo_rows()
    height, breadth = iw.shape
    cats = area.shape[0]
    rows = height + 2 * hr
    _, packed = packing(height // 8, breadth)
    vmem = pl.BlockSpec(memory_space=pltpu.VMEM)
    hbm = pl.BlockSpec(memory_space=pltpu.HBM)
    relayed = max(2 * (nr // 2 - 1), 1)
    f32 = jnp.float32
    land, ice = land.T, ice.T
    writer = writer[None]
    inputs = [
        pltpu.with_memory_space_constraint(x, pltpu.HBM)
        for x in (vel, stress, wind, current, area, volume, iw, ih, land, ice, writer)
    ]
    sent = 4 * (2 * FIELDS * hr * breadth + 20 * packed * breadth + 3 * area.size)
    velocity, stresses, strips, writer = pl.pallas_call(
        functools.partial(kernel, nr, nc),
        out_shape=(
            jax.ShapeDtypeStruct(vel.shape, f32),
            jax.ShapeDtypeStruct(stress.shape, f32),
            jax.ShapeDtypeStruct((2 * cats, nr * height, breadth), f32),
            jax.ShapeDtypeStruct(writer.shape, writer.dtype),
        ),
        in_specs=[hbm] * 11,
        out_specs=(vmem,) * 4,
        scratch_shapes=[
            pltpu.VMEM(vel.shape, f32),
            pltpu.VMEM(stress.shape, f32),
            pltpu.VMEM(wind.shape, f32),
            pltpu.VMEM(current.shape, f32),
            pltpu.VMEM(iw.shape, f32),
            pltpu.VMEM(ih.shape, f32),
            pltpu.VMEM(land.shape, land.dtype),
            pltpu.VMEM(ice.shape, ice.dtype),
            pltpu.VMEM((FIELDS, height, breadth), f32),
            pltpu.VMEM((STORED, rows + 2 * PAD, breadth), f32),
            pltpu.VMEM((STORED, rows // 2 + hr + 2 * PAD, breadth), f32),
            *[pltpu.VMEM((packed, 8, breadth), f32)] * 2,
            *[pltpu.VMEM((FIELDS, hr, breadth), f32)] * 2,
            *[pltpu.VMEM((packed, 8, breadth), f32)] * 2,
            *[pltpu.VMEM((region(breadth), 8, breadth), f32)] * 4,
            pltpu.VMEM((height, breadth), f32),
            pltpu.VMEM((height, breadth), f32),
            pltpu.SemaphoreType.DMA((11,)),
            pltpu.SemaphoreType.DMA((8,)),
            pltpu.SemaphoreType.DMA((relayed,)),
            pltpu.SemaphoreType.DMA((relayed,)),
            pltpu.SemaphoreType.DMA((2 + relayed,)),
            pltpu.SemaphoreType.DMA((2 + relayed,)),
            pltpu.SemaphoreType.DMA((11,)),
            pltpu.SemaphoreType.REGULAR,
            pltpu.SemaphoreType.REGULAR,
        ],
        compiler_params=pltpu.CompilerParams(
            collective_id=0, has_side_effects=True, vmem_limit_bytes=32 * 1024 * 1024
        ),
        cost_estimate=pl.CostEstimate(
            flops=SUB * rows * breadth * 200, bytes_accessed=sent, transcendentals=0
        ),
    )(*inputs)
    restart, velocity, stresses = pl.pallas_call(
        place,
        out_shape=(
            jax.ShapeDtypeStruct((1,) + strips.shape, f32),
            jax.ShapeDtypeStruct(vel.shape, f32),
            jax.ShapeDtypeStruct(stress.shape, f32),
        ),
        in_specs=[vmem] * 4,
        out_specs=(hbm,) * 3,
        scratch_shapes=[
            pltpu.VMEM(strips.shape[1:], f32),
            pltpu.SemaphoreType.DMA((2 + 2 * cats,)),
        ],
        compiler_params=pltpu.CompilerParams(vmem_limit_bytes=4 * 1024 * 1024),
    )(strips, velocity, stresses, writer)
    return velocity, stresses, restart


def solution(mesh):
    field = P(None, "row", "col")
    flat = P("row", "col")
    return jax.shard_map(
        functools.partial(shards, mesh.shape["row"], mesh.shape["col"]),
        mesh=mesh,
        in_specs=(field,) * 6 + (flat,) * 4 + (P(),),
        out_specs=(field, field, P("row", None, None, "col")),
        check_vma=False,
    )
```

```python
import functools

import jax
import jax.numpy as jnp
from jax import lax
from jax.experimental import pallas as pl
from jax.experimental.pallas import tpu as pltpu
from jax.sharding import PartitionSpec as P

SUB = 12
PAD = 8
FIELDS = 11
STORED = 22
U, V, S, D, T, GU, GV, INERTIA, STRENGTH, HW, HH, BETA, FW, FH, *DIFFS = range(STORED)
ALPHA = INERTIA
AU, BU, AV, BV, AS, BT, AT, BD = DIFFS
TINY = 1.1754944e-38

strength_scale = 4.0
hibler_decay = 20.0
mass_rate = 16.0
water_drag = 1.0
coriolis = 0.5


def halo_rows():
    return -(-SUB // 8) * 8


def slots_of(breadth):
    return breadth // SUB


def region(breadth):
    return -(-(halo_rows() // 8) * FIELDS // slots_of(breadth))


def packing(groups, breadth):
    per, tiles, deep = slots_of(breadth), region(breadth), halo_rows() // 8
    where = {}
    for k in range(deep):
        for f in range(FIELDS):
            n = k * FIELDS + f
            where[k, f] = divmod(n, per)
            where[groups - 1 - k, f] = (tiles + n // per, n % per)
    spare = [divmod(n, per) for n in range(deep * FIELDS, tiles * per)]
    free = spare + [(tiles + t, n) for t, n in spare]
    n = 0
    for k in range(deep, groups - deep):
        for f in range(FIELDS):
            m = n - len(free)
            where[k, f] = free[n] if m < 0 else (2 * tiles + m // per, m % per)
            n += 1
    return where, 1 + max(t for t, _ in where.values())


def expand_into(mask_ref, blocks_ref):
    block_cols, block_rows = blocks_ref.shape
    height, breadth = mask_ref.shape
    tall, wide = height // block_rows, breadth // block_cols
    counted = blocks_ref[...].astype(jnp.float32)
    start = wide * lax.broadcasted_iota(jnp.int32, (block_cols, breadth), 0)
    lane = lax.broadcasted_iota(jnp.int32, (block_cols, breadth), 1)
    inside = (lane >= start) & (lane < start + wide)
    for b in range(block_rows):
        spread = jnp.where(inside, counted[:, b : b + 1], 0.0)
        line = jnp.sum(spread, axis=0, keepdims=True)
        mask_ref[b * tall : (b + 1) * tall, :] = jnp.broadcast_to(line, (tall, breadth))


def kernel(
    nr,
    nc,
    vel_in,
    str_in,
    wind_in,
    cur_in,
    area_in,
    vol_in,
    iw_in,
    ih_in,
    land_in,
    ice_in,
    writer_in,
    vel_out,
    str_out,
    strips,
    writer_out,
    vel_ref,
    str_ref,
    wind_ref,
    cur_ref,
    iw_ref,
    ih_ref,
    land_ref,
    ice_ref,
    vals,
    main,
    side,
    pack_e,
    pack_w,
    land_n,
    land_s,
    mid_e,
    mid_w,
    low_e,
    low_w,
    high_e,
    high_w,
    ocean_ref,
    icy_ref,
    send_sem,
    recv_sem,
    x_send,
    x_recv,
    f_send,
    f_recv,
    in_sem,
    strip_sem,
    ring_sem,
):
    hr = halo_rows()
    height, breadth = iw_ref.shape
    cats = area_in.shape[0]
    rows = height + 2 * hr
    deep = hr // 8
    groups = height // 8
    total = rows // 8
    half = breadth // 2
    skip = total // 2 - deep
    tall = total - skip
    base = breadth - half + SUB
    cut = (base + breadth - SUB) // 2
    where, _ = packing(groups, breadth)
    tiles = region(breadth)
    r = lax.axis_index("row")
    c = lax.axis_index("col")
    east = lax.rem(c + 1, nc)
    west = lax.rem(c + nc - 1, nc)
    mirror = nc - 1 - c
    m_e = lax.rem(mirror + nc - 1, nc)
    m_w = lax.rem(mirror + 1, nc)
    partner = r + 1 - 2 * lax.rem(r, 2)
    is_top = r == nr - 1
    not_top = r < nr - 1
    above_bottom = r > 0
    self_e = jnp.logical_and(is_top, m_e == c)
    self_w = jnp.logical_and(is_top, m_w == c)
    other_e = jnp.logical_and(is_top, m_e != c)
    other_w = jnp.logical_and(is_top, m_w != c)
    others = [lax.rem(r + 2 * k, nr) for k in range(1, nr // 2)]

    own = pl.ds(pl.multiple_of(r * height, height), height)
    area_own = strips.at[0:cats, own, :]
    vol_own = strips.at[cats : 2 * cats, own, :]
    inputs = (
        (area_in, area_own),
        (vol_in, vol_own),
        (land_in, land_ref),
        (ice_in, ice_ref),
        (vel_in, vel_ref),
        (str_in, str_ref),
        (wind_in, wind_ref),
        (cur_in, cur_ref),
        (iw_in, iw_ref),
        (ih_in, ih_ref),
        (writer_in, writer_out),
    )
    arriving = [
        pltpu.make_async_copy(src, dst, in_sem.at[n]) for n, (src, dst) in enumerate(inputs)
    ]
    for copy in arriving:
        copy.start()

    barrier = pltpu.get_barrier_semaphore()

    def signal(semaphore, row, col):
        pl.semaphore_signal(
            semaphore,
            inc=1,
            device_id={"row": row, "col": col},
            device_id_type=pl.DeviceIdType.MESH,
        )

    odd = lax.rem(r, 2) == 1
    even = lax.rem(r, 2) == 0
    floor = r - lax.rem(r, 2)
    up_chip = jnp.logical_and(odd, not_top)
    down_chip = jnp.logical_and(even, above_bottom)
    along_x = jnp.logical_or(up_chip, down_chip)
    for n in range(nr // 2):
        chief = 2 * n + 1

        @pl.when(r != chief)
        def _():
            signal(barrier, chief, c)

    for beside in (east, west):
        signal(barrier, floor, beside)

        @pl.when(up_chip)
        def _():
            signal(barrier, r + 1, beside)

        @pl.when(down_chip)
        def _():
            signal(barrier, r - 2, beside)

    @pl.when(is_top)
    def _():
        signal(barrier, floor, mirror)

    @pl.when(other_e)
    def _():
        signal(barrier, floor, m_e)

    @pl.when(other_w)
    def _():
        signal(barrier, floor, m_w)

    def remote(src, dst, send, recv, row, col):
        return pltpu.make_async_remote_copy(
            src_ref=src,
            dst_ref=dst,
            send_sem=send,
            recv_sem=recv,
            device_id={"row": row, "col": col},
            device_id_type=pl.DeviceIdType.MESH,
        )

    snapshot = (area_own, vol_own)
    crossing = []
    for k, other in enumerate(others):
        for part, ref in enumerate(snapshot):
            n = 2 * k + part
            crossing.append(remote(ref, ref, x_send.at[n], x_recv.at[n], other, c))
    forwards = [
        remote(ref, ref, f_send.at[part], f_recv.at[part], partner, c)
        for part, ref in enumerate(snapshot)
    ]

    lane = lax.broadcasted_iota(jnp.int32, (8, breadth), 1)
    sub = lax.broadcasted_iota(jnp.int32, (8, breadth), 0)
    zero = jnp.zeros((8, breadth), jnp.float32)
    left_half = lane < half
    for f in range(5):
        for ref, end in ((main, PAD + rows), (side, PAD + 8 * tall)):
            ref[f, 0:PAD, :] = zero
            ref[f, end : end + PAD, :] = zero

    def roll(value, shift):
        shift = shift % breadth
        return pltpu.roll(value, shift, 1) if shift else value

    @pl.when(odd)
    def _():
        pl.semaphore_wait(barrier, nr - 1)
        signal(strip_sem, partner, c)

    for copy in arriving[:2]:
        copy.wait()

    @pl.when(jnp.logical_and(odd, jnp.logical_not(along_x)))
    def _():
        for copy in crossing:
            copy.start()

    @pl.when(odd)
    def _():
        for copy in forwards:
            copy.start()

    for copy in arriving[2:]:
        copy.wait()
    def halo(slot, src, dst, row, col):
        return remote(src, dst, send_sem.at[slot], recv_sem.at[slot], row, col)

    bottom = slice(0, tiles)
    upper = slice(tiles, 2 * tiles)
    vals_top = vals.at[:, height - hr : height, :]
    vals_bottom = vals.at[:, 0:hr, :]
    to_west = halo(0, pack_w, mid_e, r, west)
    to_east = halo(1, pack_e, mid_w, r, east)
    up = [
        halo(2, vals_top, land_s, r + 1, c),
        halo(4, pack_w.at[upper], low_e, r + 1, west),
        halo(5, pack_e.at[upper], low_w, r + 1, east),
    ]
    down = [
        halo(3, vals_bottom, land_n, r - 1, c),
        halo(6, pack_w.at[bottom], high_e, r - 1, west),
        halo(7, pack_e.at[bottom], high_w, r - 1, east),
    ]
    over = remote(vals_top, land_n, send_sem.at[8], recv_sem.at[3], r, mirror)
    over_w = remote(pack_w.at[upper], high_e, send_sem.at[9], recv_sem.at[6], r, m_w)
    over_e = remote(pack_e.at[upper], high_w, send_sem.at[10], recv_sem.at[7], r, m_e)

    expand_into(ocean_ref, land_ref)
    expand_into(icy_ref, ice_ref)
    packed_e, packed_w, first_e = {}, {}, {}
    order = list(range(deep)) + list(range(groups - 1, groups - 1 - deep, -1))
    order += list(range(deep, groups - deep))
    for k in order:
        here = slice(8 * k, 8 * k + 8)
        lines = pl.ds(pl.multiple_of(r * height + 8 * k, 8), 8)
        area = strips[0, lines, :]
        volume = strips[cats, lines, :]
        for n in range(1, cats):
            area = area + strips[n, lines, :]
            volume = volume + strips[cats + n, lines, :]
        ocean = ocean_ref[here, :]
        icy = icy_ref[here, :]
        strength = strength_scale * volume * jnp.exp(-hibler_decay * (1.0 - area)) * ocean
        inertia = mass_rate * (1.0 + volume)
        turning = coriolis * (1.0 + volume)
        damped = inertia + water_drag
        moving = ocean * icy
        live = moving / (damped * damped + turning * turning)
        ca = damped * live
        cb = turning * live
        rest = ocean * (1.0 - icy)
        cu = cur_ref[0, here, :]
        cv = cur_ref[1, here, :]
        gu = wind_ref[0, here, :] + water_drag * cu
        gv = wind_ref[1, here, :] + water_drag * cv
        s1, s2 = str_ref[0, here, :], str_ref[1, here, :]
        values = [
            vel_ref[0, here, :],
            vel_ref[1, here, :],
            s1 + s2,
            s1 - s2,
            2.0 * str_ref[2, here, :],
            ca * gu + cb * gv + rest * cu,
            ca * gv - cb * gu + rest * cv,
            moving * inertia,
            strength * (1.0 / 3.0),
            0.5 * iw_ref[here, :],
            0.5 * ih_ref[here, :],
        ]
        for f, value in enumerate(values):
            vals[f, here, :] = value
            t, n = where[k, f]
            at = n * SUB
            turned = roll(value, at)
            packed_w[t] = jnp.where(lane >= at, turned, packed_w[t]) if t in packed_w else turned
            if n:
                packed_e[t] = jnp.where(lane >= at - SUB, turned, packed_e[t])
            else:
                packed_e[t] = first_e[t] = turned
    for t in packed_w:
        pack_w[t] = packed_w[t]
        pack_e[t] = jnp.where(lane >= breadth - SUB, first_e[t], packed_e[t])

    @pl.when(even)
    def _():
        pl.semaphore_wait(strip_sem, 1)

    @pl.when(not_top)
    def _():
        up[0].start()

    @pl.when(above_bottom)
    def _():
        down[0].start()

    @pl.when(jnp.logical_and(even, jnp.logical_not(along_x)))
    def _():
        for copy in crossing:
            copy.start()

    @pl.when(even)
    def _():
        for copy in forwards:
            copy.start()

    @pl.when(even)
    def _():
        top_chip = (r == nr - 2).astype(jnp.int32)
        peers = 4 + 2 * above_bottom.astype(jnp.int32) + 2 - 2 * top_chip + top_chip
        peers = peers + top_chip * (m_e != c).astype(jnp.int32)
        peers = peers + top_chip * (m_w != c).astype(jnp.int32)
        pl.semaphore_wait(barrier, peers)
        signal(ring_sem, partner, c)

    @pl.when(odd)
    def _():
        pl.semaphore_wait(ring_sem, 1)

    @pl.when(self_w)
    def _():
        high_e[...] = pack_w[upper]

    @pl.when(self_e)
    def _():
        high_w[...] = pack_e[upper]

    def send_beside(mid, across, other, folded):
        mid.start()

        @pl.when(not_top)
        def _():
            up[across].start()

        @pl.when(above_bottom)
        def _():
            down[across].start()

        @pl.when(other)
        def _():
            folded.start()

    odd_col = lax.rem(c, 2) == 1

    @pl.when(odd_col)
    def _():
        send_beside(to_east, 2, other_e, over_e)

    send_beside(to_west, 1, other_w, over_w)

    @pl.when(jnp.logical_not(odd_col))
    def _():
        send_beside(to_east, 2, other_e, over_e)

    @pl.when(is_top)
    def _():
        over.start()

    @pl.when(along_x)
    def _():
        for copy in crossing:
            copy.start()

    def tile(g):
        return slice(PAD + 8 * g, PAD + 8 * g + 8)

    def homes(g):
        return [(b, n) for b, n in ((g, 0), (g - skip, 1)) if 0 <= b < tall]

    def fill(g, f, value):
        main[f, tile(g), :] = roll(value, SUB)
        for b, right in homes(g):
            mask = lane >= half if right else left_half
            pltpu.store(side.at[f, tile(b), :], roll(value, right * half - base), mask=mask)

    for k in range(groups):
        for f in range(FIELDS):
            fill(deep + k, f, vals[f, 8 * k : 8 * k + 8, :])

    @pl.when(r == 0)
    def _():
        land_s[...] = jnp.zeros(land_s.shape, jnp.float32)
        low_e[...] = jnp.zeros(low_e.shape, jnp.float32)
        low_w[...] = jnp.zeros(low_w.shape, jnp.float32)

    swap = is_top.astype(jnp.int32)

    @pl.when(above_bottom)
    def _():
        up[0].wait_recv()

    @pl.when(not_top)
    def _():
        down[0].wait_recv()

    @pl.when(is_top)
    def _():
        over.wait_recv()

    for g in range(deep):
        line = g + swap * (deep - 1 - 2 * g)
        from_n = pl.ds(pl.multiple_of(8 * line, 8), 8)
        for f in range(FIELDS):
            fill(g, f, land_s[f, 8 * g : 8 * g + 8, :])
            fill(deep + groups + g, f, land_n[f, from_n, :])

    def edges(span, source, first, origin):
        for g in span:
            for f in range(FIELDS):
                t, n = where[g - origin, f]
                yield g, f, source[t - first], n * SUB

    lows, mids = range(deep), range(deep, deep + groups)
    highs = range(deep + groups, total)
    spans = ((mids, 0, deep), (lows, tiles, deep - groups), (highs, 0, deep + groups))
    turn = coriolis / mass_rate

    def derive(ref, here):
        inertia = ref[INERTIA, here, :]
        damped = inertia + water_drag
        turning = turn * inertia
        scaled = inertia / (damped * damped + turning * turning)
        inverse = 0.5 / jnp.maximum(inertia, 1.0)
        ref[ALPHA, here, :] = damped * scaled
        ref[BETA, here, :] = turning * scaled
        ref[FW, here, :] = inverse * ref[HW, here, :]
        ref[FH, here, :] = inverse * ref[HH, here, :]

    def await_low(n):
        @pl.when(above_bottom)
        def _():
            up[n].wait_recv()

    def await_high(n, other, folded):
        @pl.when(not_top)
        def _():
            down[n].wait_recv()

        @pl.when(other)
        def _():
            folded.wait_recv()

    to_west.wait_recv()
    await_low(1)
    await_high(1, other_w, over_w)
    for source, span in zip((mid_e, low_e, high_e), spans):
        for g, f, value, at in edges(span[0], source, *span[1:]):
            for b, right in homes(g):
                to = right * half + half - SUB
                mask = (lane >= to) & (lane < to + SUB)
                pltpu.store(side.at[f, tile(b), :], roll(value, to - at), mask=mask)
    for b in range(tall):
        derive(side, tile(b))

    for n, (source, span) in enumerate(zip((mid_w, low_w, high_w), spans)):
        if n == 0:
            to_east.wait_recv()
        elif n == 1:
            await_low(2)
        else:
            await_high(2, other_e, over_e)
        for g, f, value, at in edges(span[0], source, *span[1:]):
            pltpu.store(main.at[f, tile(g), :], roll(value, SUB - at), mask=lane < SUB)
        for g in span[0]:
            derive(main, tile(g))

    near = deep + groups
    near_first = PAD + 8 * near
    own_top = near_first - 1
    shift = 8 * skip
    fold_south = (sub == 0) & is_top
    fold_north = (sub == 7) & is_top
    fold_south_side = fold_south & (lane >= half)
    fold_north_side = fold_north & (lane >= half)
    last_line = sub == 7

    def spread(ref, f, at):
        return jnp.broadcast_to(ref[f, at : at + 1, :], (8, breadth))

    def differ_velocity(ref, g):
        here = tile(g)
        u, v = ref[U, here, :], ref[V, here, :]
        wu, wv = pltpu.roll(u, 1, 1), pltpu.roll(v, 1, 1)
        ref[AU, here, :] = u - wu
        ref[BU, here, :] = u + wu
        ref[AV, here, :] = v - wv
        ref[BV, here, :] = v + wv

    def stress_tile(ref, g, folded, far):
        here = tile(g)
        south = slice(PAD + 8 * g - 1, PAD + 8 * g + 7)
        below = [ref[f, south, :] for f in (AU, BU, AV, BV)]
        if folded is not None:
            below = [
                jnp.where(folded, spread(ref, f, far), x)
                for f, x in zip((AU, BU, AV, BV), below)
            ]
        du, eu = ref[AU, here, :] + below[0], ref[BU, here, :] - below[1]
        dv, ev = ref[AV, here, :] + below[2], ref[BV, here, :] - below[3]
        hw, hh = ref[HW, here, :], ref[HH, here, :]
        gux, gvy = hw * du, hh * ev
        div, ten, shear = gux + gvy, gux - gvy, hw * dv + hh * eu
        ten4, shear4 = 0.25 * ten, 0.25 * shear
        square = div * div + (ten4 * ten + shear4 * shear)
        deform = square * lax.rsqrt(jnp.maximum(square, TINY))
        w = ref[STRENGTH, here, :] / (deform + 0.5)
        c = div - deform
        s = ref[S, here, :] * (2.0 / 3.0) + w * (c + ten4)
        d = ref[D, here, :] * (2.0 / 3.0) + w * (c - ten4)
        t = ref[T, here, :] * (2.0 / 3.0) + w * shear4
        ref[S, here, :] = s
        ref[D, here, :] = d
        ref[T, here, :] = t
        back = breadth - 1
        es, ed, et = pltpu.roll(s, back, 1), pltpu.roll(d, back, 1), pltpu.roll(t, back, 1)
        ref[AS, here, :] = es - s
        ref[BT, here, :] = et + t
        ref[AT, here, :] = et - t
        ref[BD, here, :] = ed + d

    def velocity_tile(ref, g, folded=None, ghost=None, last=None):
        here = tile(g)
        north = slice(PAD + 8 * g + 1, PAD + 8 * g + 9)
        kinds = AS, BT, AT, BD
        above = [ref[f, north, :] for f in kinds]
        if last is not None:
            above = [jnp.where(last_line, spread(ref, f, last), x) for f, x in zip(kinds, above)]
        if folded is not None:
            above = [jnp.where(folded, line, x) for line, x in zip(ghost, above)]
        es, et = above[0] + ref[AS, here, :], above[1] - ref[BT, here, :]
        ft, fd = above[2] + ref[AT, here, :], above[3] - ref[BD, here, :]
        fw, fh = ref[FW, here, :], ref[FH, here, :]
        x = ref[U, here, :] + (fw * es + fh * et)
        y = ref[V, here, :] + (fw * ft + fh * fd)
        alpha, beta = ref[ALPHA, here, :], ref[BETA, here, :]
        ref[U, here, :] = alpha * x + beta * y + ref[GU, here, :]
        ref[V, here, :] = alpha * y - beta * x + ref[GV, here, :]

    def mirrored(reach, line):
        index = reach - lane
        return jnp.take_along_axis(line, jnp.where(index < 0, index + breadth, index), axis=1)

    from_side = lane <= breadth - 1 + SUB - cut
    from_side_e = lane < breadth - 1 + SUB - cut

    def fold():
        def stack(ref, back):
            lines = [
                ref[f, at - back : at - back + 1, :]
                for at in (own_top, own_top + 8)
                for f in (S, D, T)
            ]
            return jnp.concatenate(lines + lines[:2], axis=0)

        a, b = stack(main, 0), stack(side, shift)
        last = breadth - 1
        turned, turned_e = mirrored(last, a), mirrored(last - 1, a)
        moved, moved_e = mirrored(last + 2 * SUB, a), mirrored(last - 1 + 2 * SUB, a)
        sides, sides_e = mirrored(last, b), mirrored(last - 1, b)
        moved = jnp.where(from_side, sides, moved)
        moved_e = jnp.where(from_side_e, sides_e, moved_e)
        found = []
        for here, far in ((moved, moved_e), (turned, turned_e)):
            less, more = far - here, far + here
            for first in (3, 0):
                picked = ((less, 0), (more, 2), (less, 2), (more, 1))
                found.append(
                    [
                        jnp.broadcast_to(x[first + f : first + f + 1, :], (8, breadth))
                        for x, f in picked
                    ]
                )
        return found

    def cycle(first, stresses, velocities):
        inner = range(first, tall - first)
        for g in range(first, stresses):
            differ_velocity(main, g)
            if g in inner:
                differ_velocity(side, g)
        for g in range(first, stresses):
            far = near_first + 15
            stress_tile(main, g, fold_south if g == near else None, far)
            if g in inner:
                on = fold_south_side if g == near - skip else None
                stress_tile(side, g, on, far - shift)
        ghosts = fold()
        for g in range(first, velocities):
            if g in (near - 1, near):
                velocity_tile(main, g, fold_north, ghosts[g - near + 1])
            else:
                velocity_tile(main, g, last=near_first if g == total - 1 else None)
            b = g + skip
            if g not in inner:
                continue
            if b in (near - 1, near):
                velocity_tile(side, g, fold_north_side, ghosts[2 + b - near + 1])
            else:
                last = near_first - shift if g == tall - 1 else None
                velocity_tile(side, g, last=last)

    def repeat(times, unroll, *ranges, final=None):
        def body(_, carry):
            for n in range(unroll):
                cycle(*(ranges if n < unroll - 1 or not final else final))
            return carry

        if times == unroll:
            body(0, 0)
        else:
            lax.fori_loop(0, times // unroll, body, 0)

    def relay(k, part):
        source = lax.rem(r + nr - 2 * (k + 1), nr)
        lines = pl.ds(pl.multiple_of(source * height, height), height)
        block = strips.at[part * cats : (part + 1) * cats, lines, :]
        slot = 2 + 2 * k + part
        return remote(block, block, f_send.at[slot], f_recv.at[slot], partner, c)

    relays = [relay(k, part) for k in range(len(others)) for part in range(2)]

    def pass_on(parts, early):
        for k in range(len(others)):
            source = lax.rem(r + nr - 2 * (k + 1), nr)
            outer = jnp.logical_or(source == 0, source == nr - 1)

            @pl.when(outer if early else jnp.logical_not(outer))
            def _():
                for part in parts:
                    crossing[2 * k + part].wait_recv()
                    relays[2 * k + part].start()

    wide = SUB - 8
    inside = (1, total - 1, total - 1)
    repeat(wide, 2, 0, total, total)
    pass_on((0, 1), True)
    repeat(4, 2, *inside)
    pass_on((0, 1), False)
    repeat(SUB - wide - 4, 4, *inside, final=(1, total - 1, near))

    keep = lane < cut
    for k in range(groups):
        b, right = homes(deep + k)[-1 if 2 * k >= groups else 0]
        out = []
        for f in (U, V, S, D, T):
            a = roll(main[f, tile(deep + k), :], -SUB)
            z = roll(side[f, tile(b), :], base - right * half)
            out.append(jnp.where(keep, a, z))
        at = slice(8 * k, 8 * k + 8)
        vel_out[0, at, :] = out[0]
        vel_out[1, at, :] = out[1]
        str_out[0, at, :] = 0.5 * (out[2] + out[3])
        str_out[1, at, :] = 0.5 * (out[2] - out[3])
        str_out[2, at, :] = 0.5 * out[4]

    to_west.wait_send()
    to_east.wait_send()

    @pl.when(not_top)
    def _():
        for copy in up:
            copy.wait_send()

    @pl.when(above_bottom)
    def _():
        for copy in down:
            copy.wait_send()

    @pl.when(is_top)
    def _():
        over.wait_send()

    @pl.when(other_w)
    def _():
        over_w.wait_send()

    @pl.when(other_e)
    def _():
        over_e.wait_send()

    for copy in crossing:
        copy.wait_send()
    for copy in forwards + relays:
        copy.wait()


def place(strips, vel, stress, writer, restart_out, vel_out, str_out, blank, sem):
    r = lax.axis_index("row")
    c = lax.axis_index("col")
    small = [
        pltpu.make_async_copy(vel, vel_out, sem.at[0]),
        pltpu.make_async_copy(stress, str_out, sem.at[1]),
    ]
    for copy in small:
        copy.start()
    index = lax.broadcasted_iota(jnp.int32, writer.shape, 1)
    chosen = jnp.sum(jnp.where(index == c, writer[...], 0))
    fields = strips.shape[0]

    @pl.when(chosen == r)
    def _():
        copies = [
            pltpu.make_async_copy(strips.at[n], restart_out.at[0, n], sem.at[2 + n])
            for n in range(fields)
        ]
        for copy in copies:
            copy.start()
        for copy in copies:
            copy.wait()

    @pl.when(chosen != r)
    def _():
        blank[...] = jnp.zeros(blank.shape, blank.dtype)
        copies = [
            pltpu.make_async_copy(blank, restart_out.at[0, n], sem.at[2 + n])
            for n in range(fields)
        ]
        for copy in copies:
            copy.start()
        for copy in copies:
            copy.wait()

    for copy in small:
        copy.wait()


def shards(nr, nc, *operands):
    (vel, stress, wind, current, area, volume, iw, ih, land, ice, writer) = operands
    hr = halo_rows()
    height, breadth = iw.shape
    cats = area.shape[0]
    rows = height + 2 * hr
    _, packed = packing(height // 8, breadth)
    vmem = pl.BlockSpec(memory_space=pltpu.VMEM)
    hbm = pl.BlockSpec(memory_space=pltpu.HBM)
    relayed = max(2 * (nr // 2 - 1), 1)
    f32 = jnp.float32
    land, ice = land.T, ice.T
    writer = writer[None]
    inputs = [
        pltpu.with_memory_space_constraint(x, pltpu.HBM)
        for x in (vel, stress, wind, current, area, volume, iw, ih, land, ice, writer)
    ]
    sent = 4 * (2 * FIELDS * hr * breadth + 20 * packed * breadth + 3 * area.size)
    velocity, stresses, strips, writer = pl.pallas_call(
        functools.partial(kernel, nr, nc),
        out_shape=(
            jax.ShapeDtypeStruct(vel.shape, f32),
            jax.ShapeDtypeStruct(stress.shape, f32),
            jax.ShapeDtypeStruct((2 * cats, nr * height, breadth), f32),
            jax.ShapeDtypeStruct(writer.shape, writer.dtype),
        ),
        in_specs=[hbm] * 11,
        out_specs=(vmem,) * 4,
        scratch_shapes=[
            pltpu.VMEM(vel.shape, f32),
            pltpu.VMEM(stress.shape, f32),
            pltpu.VMEM(wind.shape, f32),
            pltpu.VMEM(current.shape, f32),
            pltpu.VMEM(iw.shape, f32),
            pltpu.VMEM(ih.shape, f32),
            pltpu.VMEM(land.shape, land.dtype),
            pltpu.VMEM(ice.shape, ice.dtype),
            pltpu.VMEM((FIELDS, height, breadth), f32),
            pltpu.VMEM((STORED, rows + 2 * PAD, breadth), f32),
            pltpu.VMEM((STORED, rows // 2 + hr + 2 * PAD, breadth), f32),
            *[pltpu.VMEM((packed, 8, breadth), f32)] * 2,
            *[pltpu.VMEM((FIELDS, hr, breadth), f32)] * 2,
            *[pltpu.VMEM((packed, 8, breadth), f32)] * 2,
            *[pltpu.VMEM((region(breadth), 8, breadth), f32)] * 4,
            pltpu.VMEM((height, breadth), f32),
            pltpu.VMEM((height, breadth), f32),
            pltpu.SemaphoreType.DMA((11,)),
            pltpu.SemaphoreType.DMA((8,)),
            pltpu.SemaphoreType.DMA((relayed,)),
            pltpu.SemaphoreType.DMA((relayed,)),
            pltpu.SemaphoreType.DMA((2 + relayed,)),
            pltpu.SemaphoreType.DMA((2 + relayed,)),
            pltpu.SemaphoreType.DMA((11,)),
            pltpu.SemaphoreType.REGULAR,
            pltpu.SemaphoreType.REGULAR,
        ],
        compiler_params=pltpu.CompilerParams(
            collective_id=0, has_side_effects=True, vmem_limit_bytes=32 * 1024 * 1024
        ),
        cost_estimate=pl.CostEstimate(
            flops=SUB * rows * breadth * 200, bytes_accessed=sent, transcendentals=0
        ),
    )(*inputs)
    restart, velocity, stresses = pl.pallas_call(
        place,
        out_shape=(
            jax.ShapeDtypeStruct((1,) + strips.shape, f32),
            jax.ShapeDtypeStruct(vel.shape, f32),
            jax.ShapeDtypeStruct(stress.shape, f32),
        ),
        in_specs=[vmem] * 4,
        out_specs=(hbm,) * 3,
        scratch_shapes=[
            pltpu.VMEM(strips.shape[1:], f32),
            pltpu.SemaphoreType.DMA((2 + 2 * cats,)),
        ],
        compiler_params=pltpu.CompilerParams(vmem_limit_bytes=4 * 1024 * 1024),
    )(strips, velocity, stresses, writer)
    return velocity, stresses, restart


def solution(mesh):
    field = P(None, "row", "col")
    flat = P("row", "col")
    return jax.shard_map(
        functools.partial(shards, mesh.shape["row"], mesh.shape["col"]),
        mesh=mesh,
        in_specs=(field,) * 6 + (flat,) * 4 + (P(),),
        out_specs=(field, field, P("row", None, None, "col")),
        check_vma=False,
    )
```

```python
import functools

import jax
import jax.numpy as jnp
from jax import lax
from jax.experimental import pallas as pl
from jax.experimental.pallas import tpu as pltpu
from jax.sharding import PartitionSpec as P

SUB = 12
PAD = 8
FIELDS = 11
STORED = 23
U, V, S, D, T, GU, GV, INERTIA, STRENGTH, HW, HH, BETA, FW, FH, *DIFFS = range(STORED)
ALPHA, AU, BU, AV, BV, AS, BT, AT, BD = DIFFS
TINY = 1.1754944e-38

strength_scale = 4.0
hibler_decay = 20.0
mass_rate = 16.0
water_drag = 1.0
coriolis = 0.5


def halo_rows():
    return -(-SUB // 8) * 8


def slots_of(breadth):
    return breadth // SUB


def region(breadth):
    return -(-(halo_rows() // 8) * FIELDS // slots_of(breadth))


def packing(groups, breadth):
    per, tiles, deep = slots_of(breadth), region(breadth), halo_rows() // 8
    where = {}
    for k in range(deep):
        for f in range(FIELDS):
            n = k * FIELDS + f
            where[k, f] = divmod(n, per)
            where[groups - 1 - k, f] = (tiles + n // per, n % per)
    spare = [divmod(n, per) for n in range(deep * FIELDS, tiles * per)]
    free = spare + [(tiles + t, n) for t, n in spare]
    n = 0
    for k in range(deep, groups - deep):
        for f in range(FIELDS):
            m = n - len(free)
            where[k, f] = free[n] if m < 0 else (2 * tiles + m // per, m % per)
            n += 1
    return where, 1 + max(t for t, _ in where.values())


def expand_into(mask_ref, blocks_ref):
    block_cols, block_rows = blocks_ref.shape
    height, breadth = mask_ref.shape
    tall, wide = height // block_rows, breadth // block_cols
    counted = blocks_ref[...].astype(jnp.float32)
    start = wide * lax.broadcasted_iota(jnp.int32, (block_cols, breadth), 0)
    lane = lax.broadcasted_iota(jnp.int32, (block_cols, breadth), 1)
    inside = (lane >= start) & (lane < start + wide)
    for b in range(block_rows):
        spread = jnp.where(inside, counted[:, b : b + 1], 0.0)
        line = jnp.sum(spread, axis=0, keepdims=True)
        mask_ref[b * tall : (b + 1) * tall, :] = jnp.broadcast_to(line, (tall, breadth))


def kernel(
    nr,
    nc,
    vel_in,
    str_in,
    wind_in,
    cur_in,
    area_in,
    vol_in,
    iw_in,
    ih_in,
    land_in,
    ice_in,
    writer_in,
    vel_out,
    str_out,
    strips,
    writer_out,
    vel_ref,
    str_ref,
    wind_ref,
    cur_ref,
    iw_ref,
    ih_ref,
    land_ref,
    ice_ref,
    vals,
    main,
    side,
    pack_e,
    pack_w,
    land_n,
    land_s,
    mid_e,
    mid_w,
    low_e,
    low_w,
    high_e,
    high_w,
    ocean_ref,
    icy_ref,
    send_sem,
    recv_sem,
    x_send,
    x_recv,
    f_send,
    f_recv,
    in_sem,
    strip_sem,
    ring_sem,
):
    hr = halo_rows()
    height, breadth = iw_ref.shape
    cats = area_in.shape[0]
    rows = height + 2 * hr
    deep = hr // 8
    groups = height // 8
    total = rows // 8
    half = breadth // 2
    skip = total // 2 - deep
    tall = total - skip
    base = breadth - half + SUB
    cut = (base + breadth - SUB) // 2
    where, _ = packing(groups, breadth)
    tiles = region(breadth)
    r = lax.axis_index("row")
    c = lax.axis_index("col")
    east = lax.rem(c + 1, nc)
    west = lax.rem(c + nc - 1, nc)
    mirror = nc - 1 - c
    m_e = lax.rem(mirror + nc - 1, nc)
    m_w = lax.rem(mirror + 1, nc)
    partner = r + 1 - 2 * lax.rem(r, 2)
    is_top = r == nr - 1
    not_top = r < nr - 1
    above_bottom = r > 0
    self_e = jnp.logical_and(is_top, m_e == c)
    self_w = jnp.logical_and(is_top, m_w == c)
    other_e = jnp.logical_and(is_top, m_e != c)
    other_w = jnp.logical_and(is_top, m_w != c)
    others = [lax.rem(r + 2 * k, nr) for k in range(1, nr // 2)]

    own = pl.ds(pl.multiple_of(r * height, height), height)
    area_own = strips.at[0:cats, own, :]
    vol_own = strips.at[cats : 2 * cats, own, :]
    inputs = (
        (area_in, area_own),
        (vol_in, vol_own),
        (land_in, land_ref),
        (ice_in, ice_ref),
        (vel_in, vel_ref),
        (str_in, str_ref),
        (wind_in, wind_ref),
        (cur_in, cur_ref),
        (iw_in, iw_ref),
        (ih_in, ih_ref),
        (writer_in, writer_out),
    )
    arriving = [
        pltpu.make_async_copy(src, dst, in_sem.at[n]) for n, (src, dst) in enumerate(inputs)
    ]
    for copy in arriving:
        copy.start()

    barrier = pltpu.get_barrier_semaphore()

    def signal(semaphore, row, col):
        pl.semaphore_signal(
            semaphore,
            inc=1,
            device_id={"row": row, "col": col},
            device_id_type=pl.DeviceIdType.MESH,
        )

    odd = lax.rem(r, 2) == 1
    even = lax.rem(r, 2) == 0
    floor = r - lax.rem(r, 2)
    up_chip = jnp.logical_and(odd, not_top)
    down_chip = jnp.logical_and(even, above_bottom)
    along_x = jnp.logical_or(up_chip, down_chip)
    for n in range(nr // 2):
        chief = 2 * n + 1

        @pl.when(r != chief)
        def _():
            signal(barrier, chief, c)

    for beside in (east, west):
        signal(barrier, floor, beside)

        @pl.when(up_chip)
        def _():
            signal(barrier, r + 1, beside)

        @pl.when(down_chip)
        def _():
            signal(barrier, r - 2, beside)

    @pl.when(is_top)
    def _():
        signal(barrier, floor, mirror)

    @pl.when(other_e)
    def _():
        signal(barrier, floor, m_e)

    @pl.when(other_w)
    def _():
        signal(barrier, floor, m_w)

    def remote(src, dst, send, recv, row, col):
        return pltpu.make_async_remote_copy(
            src_ref=src,
            dst_ref=dst,
            send_sem=send,
            recv_sem=recv,
            device_id={"row": row, "col": col},
            device_id_type=pl.DeviceIdType.MESH,
        )

    snapshot = (area_own, vol_own)
    crossing = []
    for k, other in enumerate(others):
        for part, ref in enumerate(snapshot):
            n = 2 * k + part
            crossing.append(remote(ref, ref, x_send.at[n], x_recv.at[n], other, c))
    forwards = [
        remote(ref, ref, f_send.at[part], f_recv.at[part], partner, c)
        for part, ref in enumerate(snapshot)
    ]

    lane = lax.broadcasted_iota(jnp.int32, (8, breadth), 1)
    sub = lax.broadcasted_iota(jnp.int32, (8, breadth), 0)
    zero = jnp.zeros((8, breadth), jnp.float32)
    for f in range(5):
        for ref, end in ((main, PAD + rows), (side, PAD + 8 * tall)):
            ref[f, 0:PAD, :] = zero
            ref[f, end : end + PAD, :] = zero

    def roll(value, shift):
        shift = shift % breadth
        return pltpu.roll(value, shift, 1) if shift else value

    @pl.when(odd)
    def _():
        pl.semaphore_wait(barrier, nr - 1)
        signal(strip_sem, partner, c)

    for copy in arriving[:2]:
        copy.wait()

    @pl.when(jnp.logical_and(odd, jnp.logical_not(along_x)))
    def _():
        for copy in crossing:
            copy.start()

    @pl.when(odd)
    def _():
        for copy in forwards:
            copy.start()

    for copy in arriving[2:]:
        copy.wait()
    def halo(slot, src, dst, row, col):
        return remote(src, dst, send_sem.at[slot], recv_sem.at[slot], row, col)

    bottom = slice(0, tiles)
    upper = slice(tiles, 2 * tiles)
    vals_top = vals.at[:, height - SUB : height, :]
    vals_bottom = vals.at[:, 0:SUB, :]
    near_s = land_s.at[:, hr - SUB : hr, :]
    near_n = land_n.at[:, 0:SUB, :]
    near_fold = land_n.at[:, hr - SUB : hr, :]
    to_west = halo(0, pack_w, mid_e, r, west)
    to_east = halo(1, pack_e, mid_w, r, east)
    up = [
        halo(2, vals_top, near_s, r + 1, c),
        halo(4, pack_w.at[upper], low_e, r + 1, west),
        halo(5, pack_e.at[upper], low_w, r + 1, east),
    ]
    down = [
        halo(3, vals_bottom, near_n, r - 1, c),
        halo(6, pack_w.at[bottom], high_e, r - 1, west),
        halo(7, pack_e.at[bottom], high_w, r - 1, east),
    ]
    over = remote(vals_top, near_fold, send_sem.at[8], recv_sem.at[3], r, mirror)
    over_w = remote(pack_w.at[upper], high_e, send_sem.at[9], recv_sem.at[6], r, m_w)
    over_e = remote(pack_e.at[upper], high_w, send_sem.at[10], recv_sem.at[7], r, m_e)

    expand_into(ocean_ref, land_ref)
    expand_into(icy_ref, ice_ref)
    packed_e, packed_w, first_e = {}, {}, {}
    order = list(range(deep)) + list(range(groups - 1, groups - 1 - deep, -1))
    order += list(range(deep, groups - deep))
    for k in order:
        here = slice(8 * k, 8 * k + 8)
        lines = pl.ds(pl.multiple_of(r * height + 8 * k, 8), 8)
        area = strips[0, lines, :]
        volume = strips[cats, lines, :]
        for n in range(1, cats):
            area = area + strips[n, lines, :]
            volume = volume + strips[cats + n, lines, :]
        ocean = ocean_ref[here, :]
        icy = icy_ref[here, :]
        strength = strength_scale * volume * jnp.exp(-hibler_decay * (1.0 - area)) * ocean
        inertia = mass_rate * (1.0 + volume)
        turning = coriolis * (1.0 + volume)
        damped = inertia + water_drag
        moving = ocean * icy
        live = moving / (damped * damped + turning * turning)
        ca = damped * live
        cb = turning * live
        rest = ocean * (1.0 - icy)
        cu = cur_ref[0, here, :]
        cv = cur_ref[1, here, :]
        gu = wind_ref[0, here, :] + water_drag * cu
        gv = wind_ref[1, here, :] + water_drag * cv
        s1, s2 = str_ref[0, here, :], str_ref[1, here, :]
        values = [
            vel_ref[0, here, :],
            vel_ref[1, here, :],
            s1 + s2,
            s1 - s2,
            2.0 * str_ref[2, here, :],
            ca * gu + cb * gv + rest * cu,
            ca * gv - cb * gu + rest * cv,
            moving * inertia,
            strength * (1.0 / 3.0),
            0.5 * iw_ref[here, :],
            0.5 * ih_ref[here, :],
        ]
        for f, value in enumerate(values):
            vals[f, here, :] = value
            t, n = where[k, f]
            at = n * SUB
            turned = roll(value, at)
            packed_w[t] = jnp.where(lane >= at, turned, packed_w[t]) if t in packed_w else turned
            if n:
                packed_e[t] = jnp.where(lane >= at - SUB, turned, packed_e[t])
            else:
                packed_e[t] = first_e[t] = turned
    for t in packed_w:
        pack_w[t] = packed_w[t]
        pack_e[t] = jnp.where(lane >= breadth - SUB, first_e[t], packed_e[t])

    @pl.when(even)
    def _():
        pl.semaphore_wait(strip_sem, 1)

    @pl.when(not_top)
    def _():
        up[0].start()

    @pl.when(above_bottom)
    def _():
        down[0].start()

    @pl.when(jnp.logical_and(even, jnp.logical_not(along_x)))
    def _():
        for copy in crossing:
            copy.start()

    @pl.when(even)
    def _():
        for copy in forwards:
            copy.start()

    @pl.when(even)
    def _():
        top_chip = (r == nr - 2).astype(jnp.int32)
        peers = 4 + 2 * above_bottom.astype(jnp.int32) + 2 - 2 * top_chip + top_chip
        peers = peers + top_chip * (m_e != c).astype(jnp.int32)
        peers = peers + top_chip * (m_w != c).astype(jnp.int32)
        pl.semaphore_wait(barrier, peers)
        signal(ring_sem, partner, c)

    @pl.when(odd)
    def _():
        pl.semaphore_wait(ring_sem, 1)

    @pl.when(self_w)
    def _():
        high_e[...] = pack_w[upper]

    @pl.when(self_e)
    def _():
        high_w[...] = pack_e[upper]

    def send_beside(mid, across, other, folded):
        @pl.when(above_bottom)
        def _():
            down[across].start()

        mid.start()

        @pl.when(not_top)
        def _():
            up[across].start()

        @pl.when(other)
        def _():
            folded.start()

    odd_col = lax.rem(c, 2) == 1

    @pl.when(odd_col)
    def _():
        send_beside(to_east, 2, other_e, over_e)

    send_beside(to_west, 1, other_w, over_w)

    @pl.when(jnp.logical_not(odd_col))
    def _():
        send_beside(to_east, 2, other_e, over_e)

    @pl.when(is_top)
    def _():
        over.start()

    @pl.when(along_x)
    def _():
        for copy in crossing:
            copy.start()

    def tile(g):
        return slice(PAD + 8 * g, PAD + 8 * g + 8)

    def homes(g):
        return [(b, n) for b, n in ((g, 0), (g - skip, 1)) if 0 <= b < tall]

    def fill(g, f, value):
        pltpu.store(main.at[f, tile(g), :], roll(value, SUB), mask=lane >= SUB)
        for b, right in homes(g):
            mask = (lane >= half) & (lane < breadth - SUB) if right else lane < half - SUB
            pltpu.store(side.at[f, tile(b), :], roll(value, right * half - base), mask=mask)

    for k in range(groups):
        for f in range(FIELDS):
            fill(deep + k, f, vals[f, 8 * k : 8 * k + 8, :])

    @pl.when(r == 0)
    def _():
        land_s[...] = jnp.zeros(land_s.shape, jnp.float32)
        low_e[...] = jnp.zeros(low_e.shape, jnp.float32)
        low_w[...] = jnp.zeros(low_w.shape, jnp.float32)

    def fill_north(swap):
        for g in range(deep):
            line = deep - 1 - g if swap else g
            for f in range(FIELDS):
                fill(deep + groups + g, f, land_n[f, 8 * line : 8 * line + 8, :])

    @pl.when(above_bottom)
    def _():
        up[0].wait_recv()

    for g in range(deep):
        for f in range(FIELDS):
            fill(g, f, land_s[f, 8 * g : 8 * g + 8, :])

    @pl.when(not_top)
    def _():
        down[0].wait_recv()
        fill_north(False)

    def edges(span, source, first, origin):
        for g in span:
            for f in range(FIELDS):
                t, n = where[g - origin, f]
                yield g, f, source[t - first], n * SUB

    lows, mids = range(deep), range(deep, deep + groups)
    highs = range(deep + groups, total)
    spans = ((mids, 0, deep), (lows, tiles, deep - groups), (highs, 0, deep + groups))
    turn = coriolis / mass_rate

    def derive(ref, here):
        inertia = ref[INERTIA, here, :]
        damped = inertia + water_drag
        turning = turn * inertia
        scaled = inertia / (damped * damped + turning * turning)
        inverse = 0.5 / jnp.maximum(inertia, 1.0)
        ref[ALPHA, here, :] = damped * scaled
        ref[BETA, here, :] = turning * scaled
        ref[FW, here, :] = inverse * ref[HW, here, :]
        ref[FH, here, :] = inverse * ref[HH, here, :]

    def await_low(n):
        @pl.when(above_bottom)
        def _():
            up[n].wait_recv()

    def await_high(n, other, folded):
        @pl.when(not_top)
        def _():
            down[n].wait_recv()

        @pl.when(other)
        def _():
            folded.wait_recv()

    to_west.wait_recv()
    await_low(1)
    await_high(1, other_w, over_w)
    for source, span in zip((mid_e, low_e, high_e), spans):
        for g, f, value, at in edges(span[0], source, *span[1:]):
            for b, right in homes(g):
                to = right * half + half - SUB
                mask = (lane >= to) & (lane < to + SUB)
                pltpu.store(side.at[f, tile(b), :], roll(value, to - at), mask=mask)
    for b in range(tall):
        derive(side, tile(b))

    for n, (source, span) in enumerate(zip((mid_w, low_w, high_w), spans)):
        if n == 0:
            to_east.wait_recv()
        elif n == 1:
            await_low(2)
        else:
            await_high(2, other_e, over_e)
        for g, f, value, at in edges(span[0], source, *span[1:]):
            pltpu.store(main.at[f, tile(g), :], roll(value, SUB - at), mask=lane < SUB)
        for g in span[0]:
            derive(main, tile(g))

    @pl.when(is_top)
    def _():
        over.wait_recv()
        fill_north(True)
        for g in highs:
            derive(main, tile(g))
            for b, _ in homes(g):
                derive(side, tile(b))

    near = deep + groups
    near_first = PAD + 8 * near
    own_top = near_first - 1
    shift = 8 * skip
    fold_south = (sub == 0) & is_top
    fold_north = (sub == 7) & is_top
    fold_south_side = fold_south & (lane >= half)
    fold_north_side = fold_north & (lane >= half)
    last_line = sub == 7

    def spread(ref, f, at):
        return jnp.broadcast_to(ref[f, at : at + 1, :], (8, breadth))

    def differ_velocity(ref, g):
        here = tile(g)
        u, v = ref[U, here, :], ref[V, here, :]
        wu, wv = pltpu.roll(u, 1, 1), pltpu.roll(v, 1, 1)
        ref[AU, here, :] = u - wu
        ref[BU, here, :] = u + wu
        ref[AV, here, :] = v - wv
        ref[BV, here, :] = v + wv

    def stress_tile(ref, g, folded, far):
        here = tile(g)
        south = slice(PAD + 8 * g - 1, PAD + 8 * g + 7)
        below = [ref[f, south, :] for f in (AU, BU, AV, BV)]
        if folded is not None:
            below = [
                jnp.where(folded, spread(ref, f, far), x)
                for f, x in zip((AU, BU, AV, BV), below)
            ]
        du, eu = ref[AU, here, :] + below[0], ref[BU, here, :] - below[1]
        dv, ev = ref[AV, here, :] + below[2], ref[BV, here, :] - below[3]
        hw, hh = ref[HW, here, :], ref[HH, here, :]
        gux, gvy = hw * du, hh * ev
        div, ten, shear = gux + gvy, gux - gvy, hw * dv + hh * eu
        ten4, shear4 = 0.25 * ten, 0.25 * shear
        square = div * div + (ten4 * ten + shear4 * shear)
        deform = square * lax.rsqrt(jnp.maximum(square, TINY))
        w = ref[STRENGTH, here, :] / (deform + 0.5)
        c = div - deform
        s = ref[S, here, :] * (2.0 / 3.0) + w * (c + ten4)
        d = ref[D, here, :] * (2.0 / 3.0) + w * (c - ten4)
        t = ref[T, here, :] * (2.0 / 3.0) + w * shear4
        ref[S, here, :] = s
        ref[D, here, :] = d
        ref[T, here, :] = t
        back = breadth - 1
        es, ed, et = pltpu.roll(s, back, 1), pltpu.roll(d, back, 1), pltpu.roll(t, back, 1)
        ref[AS, here, :] = es - s
        ref[BT, here, :] = et + t
        ref[AT, here, :] = et - t
        ref[BD, here, :] = ed + d

    def velocity_tile(ref, g, folded=None, ghost=None, last=None):
        here = tile(g)
        north = slice(PAD + 8 * g + 1, PAD + 8 * g + 9)
        kinds = AS, BT, AT, BD
        above = [ref[f, north, :] for f in kinds]
        if last is not None:
            above = [jnp.where(last_line, spread(ref, f, last), x) for f, x in zip(kinds, above)]
        if folded is not None:
            above = [jnp.where(folded, line, x) for line, x in zip(ghost, above)]
        es, et = above[0] + ref[AS, here, :], above[1] - ref[BT, here, :]
        ft, fd = above[2] + ref[AT, here, :], above[3] - ref[BD, here, :]
        fw, fh = ref[FW, here, :], ref[FH, here, :]
        x = ref[U, here, :] + (fw * es + fh * et)
        y = ref[V, here, :] + (fw * ft + fh * fd)
        alpha, beta = ref[ALPHA, here, :], ref[BETA, here, :]
        ref[U, here, :] = alpha * x + beta * y + ref[GU, here, :]
        ref[V, here, :] = alpha * y - beta * x + ref[GV, here, :]

    def mirrored(reach, line):
        index = reach - lane
        return jnp.take_along_axis(line, jnp.where(index < 0, index + breadth, index), axis=1)

    from_side = lane <= breadth - 1 + SUB - cut
    from_side_e = lane < breadth - 1 + SUB - cut

    def fold():
        def stack(ref, back):
            lines = [
                ref[f, at - back : at - back + 1, :]
                for at in (own_top, own_top + 8)
                for f in (S, D, T)
            ]
            return jnp.concatenate(lines + lines[:2], axis=0)

        a, b = stack(main, 0), stack(side, shift)
        last = breadth - 1
        turned, turned_e = mirrored(last, a), mirrored(last - 1, a)
        moved, moved_e = mirrored(last + 2 * SUB, a), mirrored(last - 1 + 2 * SUB, a)
        sides, sides_e = mirrored(last, b), mirrored(last - 1, b)
        moved = jnp.where(from_side, sides, moved)
        moved_e = jnp.where(from_side_e, sides_e, moved_e)
        found = []
        for here, far in ((moved, moved_e), (turned, turned_e)):
            less, more = far - here, far + here
            for first in (3, 0):
                picked = ((less, 0), (more, 2), (less, 2), (more, 1))
                found.append(
                    [
                        jnp.broadcast_to(x[first + f : first + f + 1, :], (8, breadth))
                        for x, f in picked
                    ]
                )
        return found

    def cycle(first, stresses, velocities):
        inner = range(first, tall - first)
        for g in range(first, stresses):
            differ_velocity(main, g)
            if g in inner:
                differ_velocity(side, g)
        for g in range(first, stresses):
            far = near_first + 15
            stress_tile(main, g, fold_south if g == near else None, far)
            if g in inner:
                on = fold_south_side if g == near - skip else None
                stress_tile(side, g, on, far - shift)
        ghosts = fold()
        for g in range(first, velocities):
            if g in (near - 1, near):
                velocity_tile(main, g, fold_north, ghosts[g - near + 1])
            else:
                velocity_tile(main, g, last=near_first if g == total - 1 else None)
            b = g + skip
            if g not in inner:
                continue
            if b in (near - 1, near):
                velocity_tile(side, g, fold_north_side, ghosts[2 + b - near + 1])
            else:
                last = near_first - shift if g == tall - 1 else None
                velocity_tile(side, g, last=last)

    def repeat(times, unroll, *ranges, final=None):
        def body(_, carry):
            for n in range(unroll):
                cycle(*(ranges if n < unroll - 1 or not final else final))
            return carry

        if times == unroll:
            body(0, 0)
        else:
            lax.fori_loop(0, times // unroll, body, 0)

    def relay(k, part):
        source = lax.rem(r + nr - 2 * (k + 1), nr)
        lines = pl.ds(pl.multiple_of(source * height, height), height)
        block = strips.at[part * cats : (part + 1) * cats, lines, :]
        slot = 2 + 2 * k + part
        return remote(block, block, f_send.at[slot], f_recv.at[slot], partner, c)

    relays = [relay(k, part) for k in range(len(others)) for part in range(2)]

    def pass_on(parts, early):
        for k in range(len(others)):
            source = lax.rem(r + nr - 2 * (k + 1), nr)
            outer = jnp.logical_or(source == 0, source == nr - 1)

            @pl.when(outer if early else jnp.logical_not(outer))
            def _():
                for part in parts:
                    crossing[2 * k + part].wait_recv()
                    relays[2 * k + part].start()

    wide = SUB - 8
    inside = (1, total - 1, total - 1)
    repeat(wide, 2, 0, total, total)
    pass_on((0, 1), True)
    repeat(4, 2, *inside)
    pass_on((0, 1), False)
    repeat(SUB - wide - 4, 4, *inside, final=(1, total - 1, near))

    keep = lane < cut
    for k in range(groups):
        b, right = homes(deep + k)[-1 if 2 * k >= groups else 0]
        out = []
        for f in (U, V, S, D, T):
            a = roll(main[f, tile(deep + k), :], -SUB)
            z = roll(side[f, tile(b), :], base - right * half)
            out.append(jnp.where(keep, a, z))
        at = slice(8 * k, 8 * k + 8)
        vel_out[0, at, :] = out[0]
        vel_out[1, at, :] = out[1]
        str_out[0, at, :] = 0.5 * (out[2] + out[3])
        str_out[1, at, :] = 0.5 * (out[2] - out[3])
        str_out[2, at, :] = 0.5 * out[4]

    to_west.wait_send()
    to_east.wait_send()

    @pl.when(not_top)
    def _():
        for copy in up:
            copy.wait_send()

    @pl.when(above_bottom)
    def _():
        for copy in down:
            copy.wait_send()

    @pl.when(is_top)
    def _():
        over.wait_send()

    @pl.when(other_w)
    def _():
        over_w.wait_send()

    @pl.when(other_e)
    def _():
        over_e.wait_send()

    for copy in crossing:
        copy.wait_send()
    for copy in forwards + relays:
        copy.wait()


def place(strips, vel, stress, writer, restart_out, vel_out, str_out, blank, sem):
    r = lax.axis_index("row")
    c = lax.axis_index("col")
    small = [
        pltpu.make_async_copy(vel, vel_out, sem.at[0]),
        pltpu.make_async_copy(stress, str_out, sem.at[1]),
    ]
    for copy in small:
        copy.start()
    index = lax.broadcasted_iota(jnp.int32, writer.shape, 1)
    chosen = jnp.sum(jnp.where(index == c, writer[...], 0))
    fields = strips.shape[0]

    @pl.when(chosen == r)
    def _():
        copies = [
            pltpu.make_async_copy(strips.at[n], restart_out.at[0, n], sem.at[2 + n])
            for n in range(fields)
        ]
        for copy in copies:
            copy.start()
        for copy in copies:
            copy.wait()

    @pl.when(chosen != r)
    def _():
        blank[...] = jnp.zeros(blank.shape, blank.dtype)
        copies = [
            pltpu.make_async_copy(blank, restart_out.at[0, n], sem.at[2 + n])
            for n in range(fields)
        ]
        for copy in copies:
            copy.start()
        for copy in copies:
            copy.wait()

    for copy in small:
        copy.wait()


def shards(nr, nc, *operands):
    (vel, stress, wind, current, area, volume, iw, ih, land, ice, writer) = operands
    hr = halo_rows()
    height, breadth = iw.shape
    cats = area.shape[0]
    rows = height + 2 * hr
    _, packed = packing(height // 8, breadth)
    vmem = pl.BlockSpec(memory_space=pltpu.VMEM)
    hbm = pl.BlockSpec(memory_space=pltpu.HBM)
    relayed = max(2 * (nr // 2 - 1), 1)
    f32 = jnp.float32
    land, ice = land.T, ice.T
    writer = writer[None]
    inputs = [
        pltpu.with_memory_space_constraint(x, pltpu.HBM)
        for x in (vel, stress, wind, current, area, volume, iw, ih, land, ice, writer)
    ]
    sent = 4 * (2 * FIELDS * hr * breadth + 20 * packed * breadth + 3 * area.size)
    velocity, stresses, strips, writer = pl.pallas_call(
        functools.partial(kernel, nr, nc),
        out_shape=(
            jax.ShapeDtypeStruct(vel.shape, f32),
            jax.ShapeDtypeStruct(stress.shape, f32),
            jax.ShapeDtypeStruct((2 * cats, nr * height, breadth), f32),
            jax.ShapeDtypeStruct(writer.shape, writer.dtype),
        ),
        in_specs=[hbm] * 11,
        out_specs=(vmem,) * 4,
        scratch_shapes=[
            pltpu.VMEM(vel.shape, f32),
            pltpu.VMEM(stress.shape, f32),
            pltpu.VMEM(wind.shape, f32),
            pltpu.VMEM(current.shape, f32),
            pltpu.VMEM(iw.shape, f32),
            pltpu.VMEM(ih.shape, f32),
            pltpu.VMEM(land.shape, land.dtype),
            pltpu.VMEM(ice.shape, ice.dtype),
            pltpu.VMEM((FIELDS, height, breadth), f32),
            pltpu.VMEM((STORED, rows + 2 * PAD, breadth), f32),
            pltpu.VMEM((STORED, rows // 2 + hr + 2 * PAD, breadth), f32),
            *[pltpu.VMEM((packed, 8, breadth), f32)] * 2,
            *[pltpu.VMEM((FIELDS, hr, breadth), f32)] * 2,
            *[pltpu.VMEM((packed, 8, breadth), f32)] * 2,
            *[pltpu.VMEM((region(breadth), 8, breadth), f32)] * 4,
            pltpu.VMEM((height, breadth), f32),
            pltpu.VMEM((height, breadth), f32),
            pltpu.SemaphoreType.DMA((11,)),
            pltpu.SemaphoreType.DMA((8,)),
            pltpu.SemaphoreType.DMA((relayed,)),
            pltpu.SemaphoreType.DMA((relayed,)),
            pltpu.SemaphoreType.DMA((2 + relayed,)),
            pltpu.SemaphoreType.DMA((2 + relayed,)),
            pltpu.SemaphoreType.DMA((11,)),
            pltpu.SemaphoreType.REGULAR,
            pltpu.SemaphoreType.REGULAR,
        ],
        compiler_params=pltpu.CompilerParams(
            collective_id=0, has_side_effects=True, vmem_limit_bytes=32 * 1024 * 1024
        ),
        cost_estimate=pl.CostEstimate(
            flops=SUB * rows * breadth * 200, bytes_accessed=sent, transcendentals=0
        ),
    )(*inputs)
    restart, velocity, stresses = pl.pallas_call(
        place,
        out_shape=(
            jax.ShapeDtypeStruct((1,) + strips.shape, f32),
            jax.ShapeDtypeStruct(vel.shape, f32),
            jax.ShapeDtypeStruct(stress.shape, f32),
        ),
        in_specs=[vmem] * 4,
        out_specs=(hbm,) * 3,
        scratch_shapes=[
            pltpu.VMEM(strips.shape[1:], f32),
            pltpu.SemaphoreType.DMA((2 + 2 * cats,)),
        ],
        compiler_params=pltpu.CompilerParams(vmem_limit_bytes=4 * 1024 * 1024),
    )(strips, velocity, stresses, writer)
    return velocity, stresses, restart


def solution(mesh):
    field = P(None, "row", "col")
    flat = P("row", "col")
    return jax.shard_map(
        functools.partial(shards, mesh.shape["row"], mesh.shape["col"]),
        mesh=mesh,
        in_specs=(field,) * 6 + (flat,) * 4 + (P(),),
        out_specs=(field, field, P("row", None, None, "col")),
        check_vma=False,
    )
```

```python
import functools

import jax
import jax.numpy as jnp
from jax import lax
from jax.experimental import pallas as pl
from jax.experimental.pallas import tpu as pltpu
from jax.sharding import PartitionSpec as P

SUB = 12
PAD = 8
FIELDS = 11
STORED = 23
U, V, S, D, T, GU, GV, INERTIA, STRENGTH, HW, HH, BETA, FW, FH, *DIFFS = range(STORED)
ALPHA, AU, BU, AV, BV, AS, BT, AT, BD = DIFFS
TINY = 1.1754944e-38

strength_scale = 4.0
hibler_decay = 20.0
mass_rate = 16.0
water_drag = 1.0
coriolis = 0.5


def halo_rows():
    return -(-SUB // 8) * 8


def slots_of(breadth):
    return breadth // SUB


def region(breadth):
    return -(-(halo_rows() // 8) * FIELDS // slots_of(breadth))


def packing(groups, breadth):
    per, tiles, deep = slots_of(breadth), region(breadth), halo_rows() // 8
    where = {}
    for k in range(deep):
        for f in range(FIELDS):
            n = k * FIELDS + f
            where[k, f] = divmod(n, per)
            where[groups - 1 - k, f] = (tiles + n // per, n % per)
    spare = [divmod(n, per) for n in range(deep * FIELDS, tiles * per)]
    free = spare + [(tiles + t, n) for t, n in spare]
    n = 0
    for k in range(deep, groups - deep):
        for f in range(FIELDS):
            m = n - len(free)
            where[k, f] = free[n] if m < 0 else (2 * tiles + m // per, m % per)
            n += 1
    return where, 1 + max(t for t, _ in where.values())


def expand_into(mask_ref, blocks_ref):
    block_cols, block_rows = blocks_ref.shape
    height, breadth = mask_ref.shape
    tall, wide = height // block_rows, breadth // block_cols
    counted = blocks_ref[...].astype(jnp.float32)
    start = wide * lax.broadcasted_iota(jnp.int32, (block_cols, breadth), 0)
    lane = lax.broadcasted_iota(jnp.int32, (block_cols, breadth), 1)
    inside = (lane >= start) & (lane < start + wide)
    for b in range(block_rows):
        spread = jnp.where(inside, counted[:, b : b + 1], 0.0)
        line = jnp.sum(spread, axis=0, keepdims=True)
        mask_ref[b * tall : (b + 1) * tall, :] = jnp.broadcast_to(line, (tall, breadth))


def kernel(
    nr,
    nc,
    vel_in,
    str_in,
    wind_in,
    cur_in,
    area_in,
    vol_in,
    iw_in,
    ih_in,
    land_in,
    ice_in,
    writer_in,
    vel_out,
    str_out,
    strips,
    writer_out,
    vel_ref,
    str_ref,
    wind_ref,
    cur_ref,
    iw_ref,
    ih_ref,
    land_ref,
    ice_ref,
    vals,
    main,
    side,
    pack_e,
    pack_w,
    land_n,
    land_s,
    mid_e,
    mid_w,
    low_e,
    low_w,
    high_e,
    high_w,
    ocean_ref,
    icy_ref,
    send_sem,
    recv_sem,
    x_send,
    x_recv,
    f_send,
    f_recv,
    in_sem,
    strip_sem,
    ring_sem,
):
    hr = halo_rows()
    height, breadth = iw_ref.shape
    cats = area_in.shape[0]
    rows = height + 2 * hr
    deep = hr // 8
    groups = height // 8
    total = rows // 8
    half = breadth // 2
    skip = total // 2 - deep
    tall = total - skip
    base = breadth - half + SUB
    cut = (base + breadth - SUB) // 2
    where, _ = packing(groups, breadth)
    tiles = region(breadth)
    r = lax.axis_index("row")
    c = lax.axis_index("col")
    east = lax.rem(c + 1, nc)
    west = lax.rem(c + nc - 1, nc)
    mirror = nc - 1 - c
    m_e = lax.rem(mirror + nc - 1, nc)
    m_w = lax.rem(mirror + 1, nc)
    partner = r + 1 - 2 * lax.rem(r, 2)
    is_top = r == nr - 1
    not_top = r < nr - 1
    above_bottom = r > 0
    self_e = jnp.logical_and(is_top, m_e == c)
    self_w = jnp.logical_and(is_top, m_w == c)
    other_e = jnp.logical_and(is_top, m_e != c)
    other_w = jnp.logical_and(is_top, m_w != c)
    others = [lax.rem(r + 2 * k, nr) for k in range(1, nr // 2)]

    own = pl.ds(pl.multiple_of(r * height, height), height)
    area_own = strips.at[0:cats, own, :]
    vol_own = strips.at[cats : 2 * cats, own, :]
    inputs = (
        (area_in, area_own),
        (vol_in, vol_own),
        (land_in, land_ref),
        (ice_in, ice_ref),
        (vel_in, vel_ref),
        (str_in, str_ref),
        (wind_in, wind_ref),
        (cur_in, cur_ref),
        (iw_in, iw_ref),
        (ih_in, ih_ref),
        (writer_in, writer_out),
    )
    arriving = [
        pltpu.make_async_copy(src, dst, in_sem.at[n]) for n, (src, dst) in enumerate(inputs)
    ]
    for copy in arriving:
        copy.start()

    barrier = pltpu.get_barrier_semaphore()

    def signal(semaphore, row, col):
        pl.semaphore_signal(
            semaphore,
            inc=1,
            device_id={"row": row, "col": col},
            device_id_type=pl.DeviceIdType.MESH,
        )

    odd = lax.rem(r, 2) == 1
    even = lax.rem(r, 2) == 0
    floor = r - lax.rem(r, 2)
    up_chip = jnp.logical_and(odd, not_top)
    down_chip = jnp.logical_and(even, above_bottom)
    along_x = jnp.logical_or(up_chip, down_chip)
    for n in range(nr // 2):
        chief = 2 * n + 1

        @pl.when(r != chief)
        def _():
            signal(barrier, chief, c)

    for beside in (east, west):
        signal(barrier, floor, beside)

        @pl.when(up_chip)
        def _():
            signal(barrier, r + 1, beside)

        @pl.when(down_chip)
        def _():
            signal(barrier, r - 2, beside)

    @pl.when(is_top)
    def _():
        signal(barrier, floor, mirror)

    @pl.when(other_e)
    def _():
        signal(barrier, floor, m_e)

    @pl.when(other_w)
    def _():
        signal(barrier, floor, m_w)

    def remote(src, dst, send, recv, row, col):
        return pltpu.make_async_remote_copy(
            src_ref=src,
            dst_ref=dst,
            send_sem=send,
            recv_sem=recv,
            device_id={"row": row, "col": col},
            device_id_type=pl.DeviceIdType.MESH,
        )

    snapshot = (area_own, vol_own)
    crossing = []
    for k, other in enumerate(others):
        for part, ref in enumerate(snapshot):
            n = 2 * k + part
            crossing.append(remote(ref, ref, x_send.at[n], x_recv.at[n], other, c))
    forwards = [
        remote(ref, ref, f_send.at[part], f_recv.at[part], partner, c)
        for part, ref in enumerate(snapshot)
    ]

    lane = lax.broadcasted_iota(jnp.int32, (8, breadth), 1)
    sub = lax.broadcasted_iota(jnp.int32, (8, breadth), 0)
    zero = jnp.zeros((8, breadth), jnp.float32)
    for f in range(5):
        for ref, end in ((main, PAD + rows), (side, PAD + 8 * tall)):
            ref[f, 0:PAD, :] = zero
            ref[f, end : end + PAD, :] = zero

    def roll(value, shift):
        shift = shift % breadth
        return pltpu.roll(value, shift, 1) if shift else value

    @pl.when(odd)
    def _():
        pl.semaphore_wait(barrier, nr - 1)
        signal(strip_sem, partner, c)

    for copy in arriving[:2]:
        copy.wait()

    @pl.when(jnp.logical_and(odd, jnp.logical_not(along_x)))
    def _():
        for copy in crossing:
            copy.start()

    @pl.when(odd)
    def _():
        for copy in forwards:
            copy.start()

    for copy in arriving[2:]:
        copy.wait()
    def halo(slot, src, dst, row, col):
        return remote(src, dst, send_sem.at[slot], recv_sem.at[slot], row, col)

    bottom = slice(0, tiles)
    upper = slice(tiles, 2 * tiles)
    vals_top = vals.at[:, height - SUB : height, :]
    vals_bottom = vals.at[:, 0:SUB, :]
    near_s = land_s.at[:, hr - SUB : hr, :]
    near_n = land_n.at[:, 0:SUB, :]
    near_fold = land_n.at[:, hr - SUB : hr, :]
    to_west = halo(0, pack_w, mid_e, r, west)
    to_east = halo(1, pack_e, mid_w, r, east)
    up = [
        halo(2, vals_top, near_s, r + 1, c),
        halo(4, pack_w.at[upper], low_e, r + 1, west),
        halo(5, pack_e.at[upper], low_w, r + 1, east),
    ]
    down = [
        halo(3, vals_bottom, near_n, r - 1, c),
        halo(6, pack_w.at[bottom], high_e, r - 1, west),
        halo(7, pack_e.at[bottom], high_w, r - 1, east),
    ]
    over = remote(vals_top, near_fold, send_sem.at[8], recv_sem.at[3], r, mirror)
    over_w = remote(pack_w.at[upper], high_e, send_sem.at[9], recv_sem.at[6], r, m_w)
    over_e = remote(pack_e.at[upper], high_w, send_sem.at[10], recv_sem.at[7], r, m_e)

    expand_into(ocean_ref, land_ref)
    expand_into(icy_ref, ice_ref)
    packed_e, packed_w, first_e = {}, {}, {}
    order = list(range(deep)) + list(range(groups - 1, groups - 1 - deep, -1))
    order += list(range(deep, groups - deep))
    for k in order:
        here = slice(8 * k, 8 * k + 8)
        lines = pl.ds(pl.multiple_of(r * height + 8 * k, 8), 8)
        area = strips[0, lines, :]
        volume = strips[cats, lines, :]
        for n in range(1, cats):
            area = area + strips[n, lines, :]
            volume = volume + strips[cats + n, lines, :]
        ocean = ocean_ref[here, :]
        icy = icy_ref[here, :]
        strength = strength_scale * volume * jnp.exp(-hibler_decay * (1.0 - area)) * ocean
        inertia = mass_rate * (1.0 + volume)
        turning = coriolis * (1.0 + volume)
        damped = inertia + water_drag
        moving = ocean * icy
        live = moving / (damped * damped + turning * turning)
        ca = damped * live
        cb = turning * live
        rest = ocean * (1.0 - icy)
        cu = cur_ref[0, here, :]
        cv = cur_ref[1, here, :]
        gu = wind_ref[0, here, :] + water_drag * cu
        gv = wind_ref[1, here, :] + water_drag * cv
        s1, s2 = str_ref[0, here, :], str_ref[1, here, :]
        values = [
            vel_ref[0, here, :],
            vel_ref[1, here, :],
            s1 + s2,
            s1 - s2,
            2.0 * str_ref[2, here, :],
            ca * gu + cb * gv + rest * cu,
            ca * gv - cb * gu + rest * cv,
            moving * inertia,
            strength * (1.0 / 3.0),
            0.5 * iw_ref[here, :],
            0.5 * ih_ref[here, :],
        ]
        for f, value in enumerate(values):
            vals[f, here, :] = value
            t, n = where[k, f]
            at = n * SUB
            turned = roll(value, at)
            packed_w[t] = jnp.where(lane >= at, turned, packed_w[t]) if t in packed_w else turned
            if n:
                packed_e[t] = jnp.where(lane >= at - SUB, turned, packed_e[t])
            else:
                packed_e[t] = first_e[t] = turned
    for t in packed_w:
        pack_w[t] = packed_w[t]
        pack_e[t] = jnp.where(lane >= breadth - SUB, first_e[t], packed_e[t])

    @pl.when(even)
    def _():
        pl.semaphore_wait(strip_sem, 1)

    @pl.when(not_top)
    def _():
        up[0].start()

    @pl.when(above_bottom)
    def _():
        down[0].start()

    @pl.when(jnp.logical_and(even, jnp.logical_not(along_x)))
    def _():
        for copy in crossing:
            copy.start()

    @pl.when(even)
    def _():
        for copy in forwards:
            copy.start()

    @pl.when(even)
    def _():
        top_chip = (r == nr - 2).astype(jnp.int32)
        peers = 4 + 2 * above_bottom.astype(jnp.int32) + 2 - 2 * top_chip + top_chip
        peers = peers + top_chip * (m_e != c).astype(jnp.int32)
        peers = peers + top_chip * (m_w != c).astype(jnp.int32)
        pl.semaphore_wait(barrier, peers)
        signal(ring_sem, partner, c)

    @pl.when(odd)
    def _():
        pl.semaphore_wait(ring_sem, 1)

    @pl.when(self_w)
    def _():
        high_e[...] = pack_w[upper]

    @pl.when(self_e)
    def _():
        high_w[...] = pack_e[upper]

    def send_beside(mid, across, other, folded):
        @pl.when(above_bottom)
        def _():
            down[across].start()

        mid.start()

        @pl.when(not_top)
        def _():
            up[across].start()

        @pl.when(other)
        def _():
            folded.start()

    odd_col = lax.rem(c, 2) == 1

    @pl.when(odd_col)
    def _():
        send_beside(to_east, 2, other_e, over_e)

    send_beside(to_west, 1, other_w, over_w)

    @pl.when(jnp.logical_not(odd_col))
    def _():
        send_beside(to_east, 2, other_e, over_e)

    @pl.when(is_top)
    def _():
        over.start()

    @pl.when(along_x)
    def _():
        for copy in crossing:
            copy.start()

    def tile(g):
        return slice(PAD + 8 * g, PAD + 8 * g + 8)

    def homes(g):
        return [(b, n) for b, n in ((g, 0), (g - skip, 1)) if 0 <= b < tall]

    def fill(g, f, value):
        pltpu.store(main.at[f, tile(g), :], roll(value, SUB), mask=lane >= SUB)
        for b, right in homes(g):
            mask = (lane >= half) & (lane < breadth - SUB) if right else lane < half - SUB
            pltpu.store(side.at[f, tile(b), :], roll(value, right * half - base), mask=mask)

    for k in range(groups):
        for f in range(FIELDS):
            fill(deep + k, f, vals[f, 8 * k : 8 * k + 8, :])

    @pl.when(r == 0)
    def _():
        land_s[...] = jnp.zeros(land_s.shape, jnp.float32)
        low_e[...] = jnp.zeros(low_e.shape, jnp.float32)
        low_w[...] = jnp.zeros(low_w.shape, jnp.float32)

    def fill_north(swap):
        for g in range(deep):
            line = deep - 1 - g if swap else g
            for f in range(FIELDS):
                fill(deep + groups + g, f, land_n[f, 8 * line : 8 * line + 8, :])

    @pl.when(above_bottom)
    def _():
        up[0].wait_recv()

    for g in range(deep):
        for f in range(FIELDS):
            fill(g, f, land_s[f, 8 * g : 8 * g + 8, :])

    @pl.when(not_top)
    def _():
        down[0].wait_recv()
        fill_north(False)

    def edges(span, source, first, origin):
        for g in span:
            for f in range(FIELDS):
                t, n = where[g - origin, f]
                yield g, f, source[t - first], n * SUB

    lows, mids = range(deep), range(deep, deep + groups)
    highs = range(deep + groups, total)
    spans = ((mids, 0, deep), (lows, tiles, deep - groups), (highs, 0, deep + groups))
    turn = coriolis / mass_rate

    def derive(ref, here):
        inertia = ref[INERTIA, here, :]
        damped = inertia + water_drag
        turning = turn * inertia
        scaled = inertia / (damped * damped + turning * turning)
        inverse = 0.5 / jnp.maximum(inertia, 1.0)
        ref[ALPHA, here, :] = damped * scaled
        ref[BETA, here, :] = turning * scaled
        ref[FW, here, :] = inverse * ref[HW, here, :]
        ref[FH, here, :] = inverse * ref[HH, here, :]

    def await_low(n):
        @pl.when(above_bottom)
        def _():
            up[n].wait_recv()

    def await_high(n, other, folded):
        @pl.when(not_top)
        def _():
            down[n].wait_recv()

        @pl.when(other)
        def _():
            folded.wait_recv()

    to_west.wait_recv()
    await_low(1)
    await_high(1, other_w, over_w)
    for source, span in zip((mid_e, low_e, high_e), spans):
        for g, f, value, at in edges(span[0], source, *span[1:]):
            for b, right in homes(g):
                to = right * half + half - SUB
                mask = (lane >= to) & (lane < to + SUB)
                pltpu.store(side.at[f, tile(b), :], roll(value, to - at), mask=mask)
    for b in range(tall):
        derive(side, tile(b))

    for source, span in zip((low_w, high_w, mid_w), spans[1:] + spans[:1]):
        if source is mid_w:
            to_east.wait_recv()
        elif source is low_w:
            await_low(2)
        else:
            await_high(2, other_e, over_e)
        for g, f, value, at in edges(span[0], source, *span[1:]):
            pltpu.store(main.at[f, tile(g), :], roll(value, SUB - at), mask=lane < SUB)
        for g in span[0]:
            derive(main, tile(g))

    @pl.when(is_top)
    def _():
        over.wait_recv()
        fill_north(True)
        for g in highs:
            derive(main, tile(g))
            for b, _ in homes(g):
                derive(side, tile(b))

    near = deep + groups
    near_first = PAD + 8 * near
    own_top = near_first - 1
    shift = 8 * skip
    fold_south = (sub == 0) & is_top
    fold_north = (sub == 7) & is_top
    fold_south_side = fold_south & (lane >= half)
    fold_north_side = fold_north & (lane >= half)
    last_line = sub == 7

    def spread(ref, f, at):
        return jnp.broadcast_to(ref[f, at : at + 1, :], (8, breadth))

    def differ_velocity(ref, g):
        here = tile(g)
        u, v = ref[U, here, :], ref[V, here, :]
        wu, wv = pltpu.roll(u, 1, 1), pltpu.roll(v, 1, 1)
        ref[AU, here, :] = u - wu
        ref[BU, here, :] = u + wu
        ref[AV, here, :] = v - wv
        ref[BV, here, :] = v + wv

    def stress_tile(ref, g, folded, far):
        here = tile(g)
        south = slice(PAD + 8 * g - 1, PAD + 8 * g + 7)
        below = [ref[f, south, :] for f in (AU, BU, AV, BV)]
        if folded is not None:
            below = [
                jnp.where(folded, spread(ref, f, far), x)
                for f, x in zip((AU, BU, AV, BV), below)
            ]
        du, eu = ref[AU, here, :] + below[0], ref[BU, here, :] - below[1]
        dv, ev = ref[AV, here, :] + below[2], ref[BV, here, :] - below[3]
        hw, hh = ref[HW, here, :], ref[HH, here, :]
        gux, gvy = hw * du, hh * ev
        div, ten, shear = gux + gvy, gux - gvy, hw * dv + hh * eu
        ten4, shear4 = 0.25 * ten, 0.25 * shear
        square = div * div + (ten4 * ten + shear4 * shear)
        deform = square * lax.rsqrt(jnp.maximum(square, TINY))
        w = ref[STRENGTH, here, :] / (deform + 0.5)
        c = div - deform
        s = ref[S, here, :] * (2.0 / 3.0) + w * (c + ten4)
        d = ref[D, here, :] * (2.0 / 3.0) + w * (c - ten4)
        t = ref[T, here, :] * (2.0 / 3.0) + w * shear4
        ref[S, here, :] = s
        ref[D, here, :] = d
        ref[T, here, :] = t
        back = breadth - 1
        es, ed, et = pltpu.roll(s, back, 1), pltpu.roll(d, back, 1), pltpu.roll(t, back, 1)
        ref[AS, here, :] = es - s
        ref[BT, here, :] = et + t
        ref[AT, here, :] = et - t
        ref[BD, here, :] = ed + d

    def velocity_tile(ref, g, folded=None, ghost=None, last=None):
        here = tile(g)
        north = slice(PAD + 8 * g + 1, PAD + 8 * g + 9)
        kinds = AS, BT, AT, BD
        above = [ref[f, north, :] for f in kinds]
        if last is not None:
            above = [jnp.where(last_line, spread(ref, f, last), x) for f, x in zip(kinds, above)]
        if folded is not None:
            above = [jnp.where(folded, line, x) for line, x in zip(ghost, above)]
        es, et = above[0] + ref[AS, here, :], above[1] - ref[BT, here, :]
        ft, fd = above[2] + ref[AT, here, :], above[3] - ref[BD, here, :]
        fw, fh = ref[FW, here, :], ref[FH, here, :]
        x = ref[U, here, :] + (fw * es + fh * et)
        y = ref[V, here, :] + (fw * ft + fh * fd)
        alpha, beta = ref[ALPHA, here, :], ref[BETA, here, :]
        ref[U, here, :] = alpha * x + beta * y + ref[GU, here, :]
        ref[V, here, :] = alpha * y - beta * x + ref[GV, here, :]

    def mirrored(reach, line):
        index = reach - lane
        return jnp.take_along_axis(line, jnp.where(index < 0, index + breadth, index), axis=1)

    from_side = lane <= breadth - 1 + SUB - cut
    from_side_e = lane < breadth - 1 + SUB - cut

    def fold():
        def stack(ref, back):
            lines = [
                ref[f, at - back : at - back + 1, :]
                for at in (own_top, own_top + 8)
                for f in (S, D, T)
            ]
            return jnp.concatenate(lines + lines[:2], axis=0)

        a, b = stack(main, 0), stack(side, shift)
        last = breadth - 1
        turned, turned_e = mirrored(last, a), mirrored(last - 1, a)
        moved, moved_e = mirrored(last + 2 * SUB, a), mirrored(last - 1 + 2 * SUB, a)
        sides, sides_e = mirrored(last, b), mirrored(last - 1, b)
        moved = jnp.where(from_side, sides, moved)
        moved_e = jnp.where(from_side_e, sides_e, moved_e)
        found = []
        for here, far in ((moved, moved_e), (turned, turned_e)):
            less, more = far - here, far + here
            for first in (3, 0):
                picked = ((less, 0), (more, 2), (less, 2), (more, 1))
                found.append(
                    [
                        jnp.broadcast_to(x[first + f : first + f + 1, :], (8, breadth))
                        for x, f in picked
                    ]
                )
        return found

    def cycle(first, stresses, velocities):
        inner = range(first, tall - first)
        for g in range(first, stresses):
            differ_velocity(main, g)
            if g in inner:
                differ_velocity(side, g)
        for g in range(first, stresses):
            far = near_first + 15
            stress_tile(main, g, fold_south if g == near else None, far)
            if g in inner:
                on = fold_south_side if g == near - skip else None
                stress_tile(side, g, on, far - shift)
        ghosts = fold()
        for g in range(first, velocities):
            if g in (near - 1, near):
                velocity_tile(main, g, fold_north, ghosts[g - near + 1])
            else:
                velocity_tile(main, g, last=near_first if g == total - 1 else None)
            b = g + skip
            if g not in inner:
                continue
            if b in (near - 1, near):
                velocity_tile(side, g, fold_north_side, ghosts[2 + b - near + 1])
            else:
                last = near_first - shift if g == tall - 1 else None
                velocity_tile(side, g, last=last)

    def repeat(times, unroll, *ranges, final=None):
        def body(_, carry):
            for n in range(unroll):
                cycle(*(ranges if n < unroll - 1 or not final else final))
            return carry

        if times == unroll:
            body(0, 0)
        else:
            lax.fori_loop(0, times // unroll, body, 0)

    def relay(k, part):
        source = lax.rem(r + nr - 2 * (k + 1), nr)
        lines = pl.ds(pl.multiple_of(source * height, height), height)
        block = strips.at[part * cats : (part + 1) * cats, lines, :]
        slot = 2 + 2 * k + part
        return remote(block, block, f_send.at[slot], f_recv.at[slot], partner, c)

    relays = [relay(k, part) for k in range(len(others)) for part in range(2)]

    def pass_on(parts, early):
        for k in range(len(others)):
            source = lax.rem(r + nr - 2 * (k + 1), nr)
            outer = jnp.logical_or(source == 0, source == nr - 1)

            @pl.when(outer if early else jnp.logical_not(outer))
            def _():
                for part in parts:
                    crossing[2 * k + part].wait_recv()
                    relays[2 * k + part].start()

    wide = SUB - 8
    inside = (1, total - 1, total - 1)
    repeat(wide, 2, 0, total, total)
    pass_on((0, 1), True)
    repeat(4, 2, *inside)
    pass_on((0, 1), False)
    repeat(SUB - wide - 4, 4, *inside, final=(1, total - 1, near))

    keep = lane < cut
    for k in range(groups):
        b, right = homes(deep + k)[-1 if 2 * k >= groups else 0]
        out = []
        for f in (U, V, S, D, T):
            a = roll(main[f, tile(deep + k), :], -SUB)
            z = roll(side[f, tile(b), :], base - right * half)
            out.append(jnp.where(keep, a, z))
        at = slice(8 * k, 8 * k + 8)
        vel_out[0, at, :] = out[0]
        vel_out[1, at, :] = out[1]
        str_out[0, at, :] = 0.5 * (out[2] + out[3])
        str_out[1, at, :] = 0.5 * (out[2] - out[3])
        str_out[2, at, :] = 0.5 * out[4]

    to_west.wait_send()
    to_east.wait_send()

    @pl.when(not_top)
    def _():
        for copy in up:
            copy.wait_send()

    @pl.when(above_bottom)
    def _():
        for copy in down:
            copy.wait_send()

    @pl.when(is_top)
    def _():
        over.wait_send()

    @pl.when(other_w)
    def _():
        over_w.wait_send()

    @pl.when(other_e)
    def _():
        over_e.wait_send()

    for copy in crossing:
        copy.wait_send()
    for copy in forwards + relays:
        copy.wait()


def place(strips, vel, stress, writer, restart_out, vel_out, str_out, blank, sem):
    r = lax.axis_index("row")
    c = lax.axis_index("col")
    small = [
        pltpu.make_async_copy(vel, vel_out, sem.at[0]),
        pltpu.make_async_copy(stress, str_out, sem.at[1]),
    ]
    for copy in small:
        copy.start()
    index = lax.broadcasted_iota(jnp.int32, writer.shape, 1)
    chosen = jnp.sum(jnp.where(index == c, writer[...], 0))
    fields = strips.shape[0]

    @pl.when(chosen == r)
    def _():
        copies = [
            pltpu.make_async_copy(strips.at[n], restart_out.at[0, n], sem.at[2 + n])
            for n in range(fields)
        ]
        for copy in copies:
            copy.start()
        for copy in copies:
            copy.wait()

    @pl.when(chosen != r)
    def _():
        blank[...] = jnp.zeros(blank.shape, blank.dtype)
        copies = [
            pltpu.make_async_copy(blank, restart_out.at[0, n], sem.at[2 + n])
            for n in range(fields)
        ]
        for copy in copies:
            copy.start()
        for copy in copies:
            copy.wait()

    for copy in small:
        copy.wait()


def shards(nr, nc, *operands):
    (vel, stress, wind, current, area, volume, iw, ih, land, ice, writer) = operands
    hr = halo_rows()
    height, breadth = iw.shape
    cats = area.shape[0]
    rows = height + 2 * hr
    _, packed = packing(height // 8, breadth)
    vmem = pl.BlockSpec(memory_space=pltpu.VMEM)
    hbm = pl.BlockSpec(memory_space=pltpu.HBM)
    relayed = max(2 * (nr // 2 - 1), 1)
    f32 = jnp.float32
    land, ice = land.T, ice.T
    writer = writer[None]
    inputs = [
        pltpu.with_memory_space_constraint(x, pltpu.HBM)
        for x in (vel, stress, wind, current, area, volume, iw, ih, land, ice, writer)
    ]
    sent = 4 * (2 * FIELDS * hr * breadth + 20 * packed * breadth + 3 * area.size)
    velocity, stresses, strips, writer = pl.pallas_call(
        functools.partial(kernel, nr, nc),
        out_shape=(
            jax.ShapeDtypeStruct(vel.shape, f32),
            jax.ShapeDtypeStruct(stress.shape, f32),
            jax.ShapeDtypeStruct((2 * cats, nr * height, breadth), f32),
            jax.ShapeDtypeStruct(writer.shape, writer.dtype),
        ),
        in_specs=[hbm] * 11,
        out_specs=(vmem,) * 4,
        scratch_shapes=[
            pltpu.VMEM(vel.shape, f32),
            pltpu.VMEM(stress.shape, f32),
            pltpu.VMEM(wind.shape, f32),
            pltpu.VMEM(current.shape, f32),
            pltpu.VMEM(iw.shape, f32),
            pltpu.VMEM(ih.shape, f32),
            pltpu.VMEM(land.shape, land.dtype),
            pltpu.VMEM(ice.shape, ice.dtype),
            pltpu.VMEM((FIELDS, height, breadth), f32),
            pltpu.VMEM((STORED, rows + 2 * PAD, breadth), f32),
            pltpu.VMEM((STORED, rows // 2 + hr + 2 * PAD, breadth), f32),
            *[pltpu.VMEM((packed, 8, breadth), f32)] * 2,
            *[pltpu.VMEM((FIELDS, hr, breadth), f32)] * 2,
            *[pltpu.VMEM((packed, 8, breadth), f32)] * 2,
            *[pltpu.VMEM((region(breadth), 8, breadth), f32)] * 4,
            pltpu.VMEM((height, breadth), f32),
            pltpu.VMEM((height, breadth), f32),
            pltpu.SemaphoreType.DMA((11,)),
            pltpu.SemaphoreType.DMA((8,)),
            pltpu.SemaphoreType.DMA((relayed,)),
            pltpu.SemaphoreType.DMA((relayed,)),
            pltpu.SemaphoreType.DMA((2 + relayed,)),
            pltpu.SemaphoreType.DMA((2 + relayed,)),
            pltpu.SemaphoreType.DMA((11,)),
            pltpu.SemaphoreType.REGULAR,
            pltpu.SemaphoreType.REGULAR,
        ],
        compiler_params=pltpu.CompilerParams(
            collective_id=0, has_side_effects=True, vmem_limit_bytes=32 * 1024 * 1024
        ),
        cost_estimate=pl.CostEstimate(
            flops=SUB * rows * breadth * 200, bytes_accessed=sent, transcendentals=0
        ),
    )(*inputs)
    restart, velocity, stresses = pl.pallas_call(
        place,
        out_shape=(
            jax.ShapeDtypeStruct((1,) + strips.shape, f32),
            jax.ShapeDtypeStruct(vel.shape, f32),
            jax.ShapeDtypeStruct(stress.shape, f32),
        ),
        in_specs=[vmem] * 4,
        out_specs=(hbm,) * 3,
        scratch_shapes=[
            pltpu.VMEM(strips.shape[1:], f32),
            pltpu.SemaphoreType.DMA((2 + 2 * cats,)),
        ],
        compiler_params=pltpu.CompilerParams(vmem_limit_bytes=4 * 1024 * 1024),
    )(strips, velocity, stresses, writer)
    return velocity, stresses, restart


def solution(mesh):
    field = P(None, "row", "col")
    flat = P("row", "col")
    return jax.shard_map(
        functools.partial(shards, mesh.shape["row"], mesh.shape["col"]),
        mesh=mesh,
        in_specs=(field,) * 6 + (flat,) * 4 + (P(),),
        out_specs=(field, field, P("row", None, None, "col")),
        check_vma=False,
    )
```
